128 devices in a mesh: tau: 8 (over x, core), tile: 16 (over z, y).
Axes of the slice: x: 4, y: 4, z: 4, core: 2. Of those that a mesh axis runs over, the one named last changes fastest.
Arguments:
- occupied: bfloat16 [8, 2048, 128, 128], P('tau', 'tile'), may hold values from -6 to 6
- virtual: bfloat16 [8, 2048, 128, 128], P('tau', 'tile'), may hold values from -0.125 to 0.125
- cos_weights: float32 [4, 8], replicated, may hold values from -1 to 1
- pair_occ: int32 [3072, 16], P('tile'), may hold values from 0 to 127
- pair_virt: int32 [3072, 16], P('tile'), may hold values from 0 to 127
- partial_target_tile: int32 [3072], P('tile'), may hold values from 0 to 511, as said below
Outputs:
- spectrum: float32 [4, 512, 128, 128], P(None, 'tile', 'tau')
The draws below stay inside these ranges and needn't reach their ends.
Inputs may be any that keep to these rules, and one draw needn't show every extreme that they name: `partial_target_tile`: within each aligned block of 192 entries, no owner (values d * 32 to (d + 1) * 32 - 1 for owner d) is named more than 24 times; one owner is named exactly 24 times in every block.
All inputs are finite; a program needn't handle non-finite values.
Results may differ from the reference program's by a relative error of at most 0.0003.
Values sent between devices are 32-bit elements; how exact they have to be, the bound alone decides.
A program may use at most 192 MiB of HBM per device.

```python
import math
import jax
import jax.numpy as jnp
from jax import lax

TILE = 128
TERMS = 16
NFREQ = 4
SLOT_DEV = 128
PART_DEV = 192
CHI_DEV = 32
NTAU = 8
NOCC = 2048
NPART = 3072
NCHI = 512
CAP = 24


def draw_partial_target_tile(key, part):
    owners = NPART // PART_DEV
    first, second, third, fourth = jax.random.split(jax.random.fold_in(key, 7), 4)
    complete_holder = jax.random.randint(first, (), 0, owners)
    owner_preference = jax.random.randint(second, (owners, owners), 0, 1 << 19)
    random_perturbation = jax.random.randint(third, (owners, owners, CAP), 0, 1 << 19)
    holder_indices = jnp.arange(owners, dtype=jnp.int32)
    extra_credit = jnp.where(holder_indices == complete_holder, 1 << 20, 0).astype(jnp.int32)
    ranking_value = owner_preference[:, :, None] + random_perturbation + extra_credit[None, :, None]
    places = jnp.arange(owners * CAP, dtype=jnp.int32).reshape(owners, CAP)
    ranking_value = ranking_value * (owners * CAP) + places[None]
    flat = ranking_value.reshape(owners, owners * CAP)
    _, chosen = lax.top_k(flat, PART_DEV)
    owner = (chosen // CAP).astype(jnp.int32)
    within = jax.random.randint(fourth, (owners, PART_DEV), 0, CHI_DEV)
    return (owner * CHI_DEV + within).reshape(-1).astype(jnp.int32)


def touch_ends(drawn, stream_key, low, largest):
    longest = drawn.shape.index(max(drawn.shape))
    spots = []
    for shift in (0, 1):
        where = [jax.random.randint(jax.random.fold_in(stream_key, axis), (), 0, length) for axis, length in enumerate(drawn.shape)]
        where[longest] = (where[longest] + shift) % drawn.shape[longest]
        spots.append(tuple(where))
    return drawn.at[spots[0]].set(low).at[spots[1]].set(largest)


def level_of(rng, dims, pieces, least, largest):
    factor_of = 1.0
    for position, parts in pieces:
        draws = jax.random.uniform(jax.random.fold_in(jax.random.fold_in(rng, 6), position), (parts,), jnp.float32, least / len(pieces), largest / len(pieces))
        factor_of = factor_of * jnp.repeat(jnp.exp(draws), dims[position] // parts).reshape((-1,) + (1,) * (len(dims) - 1 - position))
    return factor_of


def noise(rng, dims, width, reach, cuts=(), held_as=jnp.bfloat16):
    array = width * jax.random.normal(rng, dims, jnp.float32)
    if cuts:
        array = array * level_of(rng, dims, cuts, -0.22, 0.18)
    return jnp.clip(array, -reach, reach).astype(held_as)


def setup_inputs(seed: int = 0) -> dict:
    splits = jax.random.split(jax.random.key(seed), 7)
    return {
        "occupied": noise(splits[0], (NTAU, NOCC, TILE, TILE), 1.0, 6.0, ((0, 8), (1, 16))),
        "virtual": noise(splits[1], (NTAU, NOCC, TILE, TILE), (TILE * TERMS) ** -0.5, 0.125, ((0, 8), (1, 16))),
        "cos_weights": jnp.clip(jax.random.uniform(splits[2], (NFREQ, NTAU), jnp.float32, -1.0, 1.0), -1.0, 1.0),
        "pair_occ": touch_ends(jax.random.randint(splits[3], (NPART, TERMS), 0, SLOT_DEV), jax.random.fold_in(splits[3], 1), 0, SLOT_DEV - 1).astype(jnp.int32),
        "pair_virt": touch_ends(jax.random.randint(splits[4], (NPART, TERMS), 0, SLOT_DEV), jax.random.fold_in(splits[4], 1), 0, SLOT_DEV - 1).astype(jnp.int32),
        "partial_target_tile": draw_partial_target_tile(jax.random.fold_in(splits[6], 71), 0),
    }


def reference(occupied, virtual, cos_weights, pair_occ, pair_virt, partial_target_tile):
    owner_base = (jnp.arange(NPART, dtype=jnp.int32) // PART_DEV) * SLOT_DEV
    occ_global = (pair_occ + owner_base[:, None]).astype(jnp.int32)
    virt_global = (pair_virt + owner_base[:, None]).astype(jnp.int32)
    group = math.gcd(NPART, 16)
    count = NPART // group
    occ_blocks = occ_global.reshape(count, group, TERMS)
    virt_blocks = virt_global.reshape(count, group, TERMS)
    dest_blocks = partial_target_tile.astype(jnp.int32).reshape(count, group)

    def time_step(spectrum, step_index):
        occ_now = lax.dynamic_index_in_dim(occupied, step_index, 0, keepdims=False)
        virt_now = lax.dynamic_index_in_dim(virtual, step_index, 0, keepdims=False)

        def add_block(chi_time, items):
            left = jnp.take(occ_now, items[0], axis=0).astype(jnp.float32)
            right = jnp.take(virt_now, items[1], axis=0).astype(jnp.float32)
            product = jnp.einsum("bjrk,bjkc->brc", left, right, precision=lax.Precision.HIGHEST)
            return chi_time.at[items[2]].add(product), None

        chi_time, _ = lax.scan(add_block, jnp.zeros((NCHI, TILE, TILE), jnp.float32),
                               (occ_blocks, virt_blocks, dest_blocks))
        weights = lax.dynamic_index_in_dim(cos_weights, step_index, 1, keepdims=False)
        return spectrum + weights[:, None, None, None] * chi_time[None], None

    spectrum, _ = lax.scan(time_step, jnp.zeros((NFREQ, NCHI, TILE, TILE), jnp.float32),
                           jnp.arange(NTAU, dtype=jnp.int32))
    return spectrum
```

```python
import functools

import jax
import jax.numpy as jnp
from jax import lax
from jax.experimental import pallas as pl
from jax.experimental.pallas import tpu as pltpu
from jax.sharding import PartitionSpec as P

CHI_DEV = 32
CAP = 24
CHUNKS = 8
PBUFS = 3
YBUFS = 2
MESH = pl.DeviceIdType.MESH


def main_kernel(ny, nz, groups, terms,
                weights, occ_idx, virt_idx, part, keep, place, occ, virt, tv,
                out,
                pbuf, xrecv, freq, ybuf, yrecv, work, dense, zrecv, trecv, tbl_v, tbl,
                x_send, x_recv, y_send, y_recv, z_send, z_recv, t_send, t_recv, tbl_sem):
    tau = lax.axis_index("tau")
    tile = lax.axis_index("tile")
    z, y = tile // ny, tile % ny
    mine = (y, z)
    sizes = (ny, nz)
    freqs, _, rows, width = out.shape
    half = freqs // 2
    per = freq.shape[0]
    slots = yrecv.shape[3]
    each = slots // ny
    rounds = CHUNKS

    def peer(h, i):
        return {"tile": z * ny + i if h == 0 else i * ny + y}

    barrier = pltpu.get_barrier_semaphore()
    for step in range(1, groups):
        pl.semaphore_signal(barrier, inc=1, device_id={"tau": (tau + step) % groups},
                            device_id_type=MESH)
    for h in range(2):
        for step in range(1, sizes[h]):
            pl.semaphore_signal(barrier, inc=1, device_id=peer(h, (mine[h] + step) % sizes[h]),
                                device_id_type=MESH)
    pl.semaphore_wait(barrier, groups - 1 + ny - 1 + nz - 1)

    def meta(h, to, at):
        return pltpu.make_async_remote_copy(
            src_ref=tv.at[h, to], dst_ref=trecv.at[h, mine[h]],
            send_sem=t_send.at[h * 4 + to], recv_sem=t_recv.at[h * 4 + at],
            device_id=peer(h, to), device_id_type=MESH)

    def x_copy(c, to, at):
        return pltpu.make_async_remote_copy(
            src_ref=pbuf.at[c % PBUFS, to], dst_ref=xrecv.at[c, tau],
            send_sem=x_send.at[c * groups + to], recv_sem=x_recv.at[c * groups + at],
            device_id={"tau": to}, device_id_type=MESH)

    def x_arrival(c, source):
        return pltpu.make_async_remote_copy(
            src_ref=pbuf.at[c % PBUFS, 0], dst_ref=xrecv.at[c, source],
            send_sem=x_send.at[c * groups], recv_sem=x_recv.at[c * groups + source],
            device_id={"tau": source}, device_id_type=MESH)

    def y_copy(c, h, to, at):
        return pltpu.make_async_remote_copy(
            src_ref=ybuf.at[c % YBUFS, h, to], dst_ref=yrecv.at[c, h, mine[h]],
            send_sem=y_send.at[c * 8 + h * 4 + to], recv_sem=y_recv.at[c * 8 + h * 4 + at],
            device_id=peer(h, to), device_id_type=MESH)

    def y_arrival(c, h, source):
        return pltpu.make_async_remote_copy(
            src_ref=ybuf.at[c % YBUFS, h, 0], dst_ref=yrecv.at[c, h, source],
            send_sem=y_send.at[c * 8 + h * 4], recv_sem=y_recv.at[c * 8 + h * 4 + source],
            device_id=peer(h, source), device_id_type=MESH)

    def z_copy(h, to, at):
        return pltpu.make_async_remote_copy(
            src_ref=dense.at[h, to], dst_ref=zrecv.at[h, mine[1 - h]],
            send_sem=z_send.at[h * 4 + to], recv_sem=z_recv.at[h * 4 + at],
            device_id=peer(1 - h, to), device_id_type=MESH)

    def z_arrival(h, source):
        return pltpu.make_async_remote_copy(
            src_ref=dense.at[h, 0], dst_ref=zrecv.at[h, source],
            send_sem=z_send.at[h * 4], recv_sem=z_recv.at[h * 4 + source],
            device_id=peer(1 - h, source), device_id_type=MESH)

    def others(h):
        return [(mine[h] + step) % sizes[h] for step in range(1, sizes[h])]

    for h in range(2):
        for to in others(h):
            meta(h, to, mine[h]).start()
        trecv[h, mine[h]] = tv[h, mine[h]]
        for s in range(sizes[h]):
            work[h, s, slots] = jnp.zeros((half, rows, width), jnp.float32)
        for o in range(sizes[1 - h]):
            @pl.loop(0, CHI_DEV)
            def _(e):
                dense[h, o, e] = jnp.zeros((half, rows, width), jnp.float32)

    def compute(c):
        slot = c % PBUFS

        def one(i, last):
            n = c * per + i
            p = part[n]
            left = [occ[occ_idx[p * terms + j]] for j in range(terms)]
            right = [virt[virt_idx[p * terms + j]] for j in range(terms)]
            acc = jnp.dot(
                jnp.concatenate(left, axis=1),
                jnp.concatenate(right, axis=0),
                preferred_element_type=jnp.float32,
            )
            acc = acc + jnp.where(keep[n] != 0, last, 0.0)
            for g in range(groups):
                pbuf[slot, g, i] = acc[g * rows:(g + 1) * rows]
            return acc

        lax.fori_loop(0, per, one, jnp.zeros((rows * groups, width), jnp.float32))

    def transform(c):
        @pl.loop(0, per)
        def _(i):
            terms_in = [xrecv[c, s, i] for s in range(groups)]
            for k in range(freqs):
                total = weights[k, 0] * terms_in[0]
                for s in range(1, groups):
                    total += weights[k, s] * terms_in[s]
                freq[i, k] = total

        @pl.loop(0, nz)
        def _(dz):
            @pl.loop(0, ny)
            def _(dy):
                for m in range(each):
                    i = place[(c * ny * nz + dz * ny + dy) * each + m]
                    ybuf[c % YBUFS, 0, dy, dz * each + m] = freq[i, 0:half]
                    ybuf[c % YBUFS, 1, dz, dy * each + m] = freq[i, half:freqs]

    def tables():
        lane = lax.broadcasted_iota(jnp.int32, (CHUNKS, width), 1)
        for h in range(2):
            for s in others(h):
                meta(h, s, s).wait_recv()
            for s in range(sizes[h]):
                found = jnp.full((CHUNKS, width), slots, jnp.int32)
                for e in range(slots):
                    found = jnp.where(trecv[h, s, e] == lane, e, found)
                tbl_v[h, s] = found
        copy = pltpu.make_async_copy(tbl_v, tbl, tbl_sem)
        copy.start()
        copy.wait()

    def densify(c):
        for h in range(2):
            for s in range(sizes[h]):
                @pl.loop(0, slots)
                def _(e):
                    work[h, s, e] = yrecv[c, h, s, e]
        for h in range(2):
            @pl.loop(0, sizes[1 - h])
            def _(o):
                @pl.loop(0, CHI_DEV, unroll=2)
                def _(e):
                    total = dense[h, o, e]
                    for s in range(sizes[h]):
                        total += work[h, s, tbl[h, s, c, o * CHI_DEV + e]]
                    dense[h, o, e] = total

    @pl.loop(0, rounds + 2)
    def _(t):
        @pl.when(t < rounds)
        def _():
            @pl.when(t >= PBUFS)
            def _():
                for step in range(1, groups):
                    to = (tau + step) % groups
                    x_copy(t - PBUFS, to, tau).wait_send()
            compute(t)
            for step in range(1, groups):
                to = (tau + step) % groups
                x_copy(t, to, tau).start()

            @pl.loop(0, per)
            def _(i):
                xrecv[t, tau, i] = pbuf[t % PBUFS, tau, i]

        @pl.when((t >= 1) & (t < rounds + 1))
        def _():
            c = t - 1

            @pl.when(c >= YBUFS)
            def _():
                for h in range(2):
                    for to in others(h):
                        y_copy(c - YBUFS, h, to, mine[h]).wait_send()
            for step in range(1, groups):
                x_arrival(c, (tau + step) % groups).wait_recv()
            transform(c)
            for h in range(2):
                for to in others(h):
                    y_copy(c, h, to, mine[h]).start()

                @pl.loop(0, slots)
                def _(e):
                    yrecv[c, h, mine[h], e] = ybuf[c % YBUFS, h, mine[h], e]

        @pl.when(t == 2)
        def _():
            tables()

        @pl.when(t >= 2)
        def _():
            c = t - 2
            for h in range(2):
                for s in others(h):
                    y_arrival(c, h, s).wait_recv()
            densify(c)

    for h in range(2):
        for to in others(1 - h):
            z_copy(h, to, mine[1 - h]).start()
    for h in range(2):
        for s in others(1 - h):
            z_arrival(h, s).wait_recv()

        own = mine[1 - h]

        @pl.loop(0, CHI_DEV)
        def _(e):
            total = dense[h, own, e]
            for s in others(1 - h):
                total += zrecv[h, s, e]
            for k in range(half):
                out[h * half + k, e] = total[k]

    for h in range(2):
        for to in others(h):
            meta(h, to, mine[h]).wait_send()
        for to in others(1 - h):
            z_copy(h, to, mine[1 - h]).wait_send()

    @pl.loop(rounds - YBUFS, rounds)
    def _(c):
        for h in range(2):
            for to in others(h):
                y_copy(c, h, to, mine[h]).wait_send()

    @pl.loop(rounds - PBUFS, rounds)
    def _(c):
        for step in range(1, groups):
            x_copy(c, (tau + step) % groups, tau).wait_send()


def plan(target, owners, ny, nz):
    count = target.shape[0]
    per = count // CHUNKS
    each = CAP // CHUNKS
    index = jnp.arange(count, dtype=jnp.int32)
    key = target * 256 + index
    rank = jnp.sum((key[None, :] < key[:, None]).astype(jnp.int32), axis=1)
    ordered = jnp.sum(jnp.where(rank[:, None] == index[None, :], key[:, None], 0), axis=0)
    ordered = ordered.reshape(per, CHUNKS).T
    part = ordered & 255
    tile = ordered >> 8
    same = (tile[:, 1:] == tile[:, :-1]).astype(jnp.int32)
    none = jnp.zeros((CHUNKS, 1), jnp.int32)
    keep = jnp.concatenate([none, same], axis=1)
    last = 1 - jnp.concatenate([same, none], axis=1)
    owner = tile // CHI_DEV
    value = jnp.where(last != 0, tile - owner * CHI_DEV, -1)
    d = jnp.arange(owners, dtype=jnp.int32)
    start = jnp.sum((owner[:, None, :] < d[None, :, None]).astype(jnp.int32), axis=2)
    place = start[:, :, None] + jnp.arange(each, dtype=jnp.int32)
    within = jnp.arange(per, dtype=jnp.int32)
    hit = (place[..., None] == within) & (owner[:, None, None, :] == d[None, :, None, None])
    goal = jnp.sum(jnp.where(hit, value[:, None, None, :] + 1, 0), axis=3) - 1
    place = jnp.minimum(place, per - 1)
    goal = goal.reshape(CHUNKS, nz, ny, each)
    zs = jnp.arange(nz, dtype=jnp.int32)[None, :, None, None] * CHI_DEV
    ys = jnp.arange(ny, dtype=jnp.int32)[None, None, :, None] * CHI_DEV
    to_y = jnp.where(goal >= 0, goal + zs, -1).transpose(2, 1, 3, 0).reshape(ny, nz * each, CHUNKS)
    to_z = jnp.where(goal >= 0, goal + ys, -1).transpose(1, 2, 3, 0).reshape(nz, ny * each, CHUNKS)
    both = jnp.stack([to_y, to_z])
    both = jnp.broadcast_to(both[..., None], both.shape + (128,))
    return part.reshape(-1), keep.reshape(-1), place.reshape(-1), both


def body(occupied, virtual, cos_weights, pair_occ, pair_virt, partial_target_tile):
    owners = lax.axis_size("tile")
    groups = lax.axis_size("tau")
    size = occupied.shape[2]
    terms = pair_occ.shape[1]
    count = partial_target_tile.shape[0]
    freqs = cos_weights.shape[0]
    ny = 1
    while 2 * ny * 2 * ny <= owners:
        ny *= 2
    nz = owners // ny
    rows = size // groups
    per = count // CHUNKS
    slots = ny * (CAP // CHUNKS)
    half = freqs // 2
    part, keep, place, both = plan(partial_target_tile, owners, ny, nz)
    smem = pl.BlockSpec(memory_space=pltpu.SMEM)
    vmem = pl.BlockSpec(memory_space=pltpu.VMEM)
    dma = pltpu.SemaphoreType.DMA
    f32 = jnp.float32
    return pl.pallas_call(
        functools.partial(main_kernel, ny, nz, groups, terms),
        out_shape=jax.ShapeDtypeStruct((freqs, CHI_DEV, rows, size), f32),
        in_specs=[smem] * 6 + [vmem] * 3,
        out_specs=vmem,
        scratch_shapes=[
            pltpu.VMEM((PBUFS, groups, per, rows, size), f32),
            pltpu.VMEM((CHUNKS, groups, per, rows, size), f32),
            pltpu.VMEM((per, freqs, rows, size), f32),
            pltpu.VMEM((YBUFS, 2, ny, slots, half, rows, size), f32),
            pltpu.VMEM((CHUNKS, 2, ny, slots, half, rows, size), f32),
            pltpu.VMEM((2, ny, slots + 1, half, rows, size), f32),
            pltpu.VMEM((2, ny, CHI_DEV, half, rows, size), f32),
            pltpu.VMEM((2, ny, CHI_DEV, half, rows, size), f32),
            pltpu.VMEM((2, ny, slots, CHUNKS, size), jnp.int32),
            pltpu.VMEM((2, ny, CHUNKS, size), jnp.int32),
            pltpu.SMEM((2, ny, CHUNKS, size), jnp.int32),
            dma((CHUNKS * groups,)),
            dma((CHUNKS * groups,)),
            dma((CHUNKS * 8,)),
            dma((CHUNKS * 8,)),
            dma((8,)),
            dma((8,)),
            dma((8,)),
            dma((8,)),
            dma,
        ],
        compiler_params=pltpu.CompilerParams(
            collective_id=0, has_side_effects=True, vmem_limit_bytes=62 * 1024 * 1024),
    )(cos_weights, pair_occ.reshape(-1), pair_virt.reshape(-1), part, keep, place,
      occupied[0], virtual[0], both)


def solution(mesh):
    in_specs = (
        P("tau", "tile", None, None),
        P("tau", "tile", None, None),
        P(),
        P("tile", None),
        P("tile", None),
        P("tile"),
    )
    out_specs = P(None, "tile", "tau", None)
    return jax.shard_map(body, mesh=mesh, in_specs=in_specs, out_specs=out_specs, check_vma=False)
```

```python
import functools
import math

import jax
import jax.numpy as jnp
from jax import lax
from jax.experimental import pallas as pl
from jax.experimental.pallas import tpu as pltpu
from jax.sharding import PartitionSpec as P

CHI_DEV = 32
CAP = 24
CHUNKS = 8
PBUFS = 3
YBUFS = 2
RING = 4
LAG = 3
MESH = pl.DeviceIdType.MESH


def main_kernel(ny, nz, groups, terms,
                weights, occ_idx, virt_idx, part, keep, place, occ, virt, tv,
                out,
                early, late, timed, x_early, x_late, freq, ybuf, yrecv, work, dense, zrecv,
                final, back, trecv, tbl_v, tbl,
                e_send, e_recv, l_send, l_recv, y_send, y_recv, z_send, z_recv,
                b_send, b_recv, t_send, t_recv, tbl_sem):
    tau = lax.axis_index("tau")
    tile = lax.axis_index("tile")
    x, core = tau // 2, tau % 2
    nx = groups // 2
    z, y = tile // ny, tile % ny
    mine = (y, z)
    sizes = (ny, nz)
    freqs, _, rows, width = out.shape
    low = rows // 2
    half = freqs // 2
    per = freq.shape[0]
    slots = yrecv.shape[4]
    each = slots // ny
    rounds = CHUNKS

    def peer(h, i):
        return {"tile": z * ny + i if h == 0 else i * ny + y}

    def others(h):
        return [(mine[h] + step) % sizes[h] for step in range(1, sizes[h])]

    def times():
        return [(tau + step) % groups for step in range(1, groups)]

    barrier = pltpu.get_barrier_semaphore()
    for to in times():
        pl.semaphore_signal(barrier, inc=1, device_id={"tau": to}, device_id_type=MESH)
    for h in range(2):
        for to in others(h):
            pl.semaphore_signal(barrier, inc=1, device_id=peer(h, to), device_id_type=MESH)
    pl.semaphore_wait(barrier, groups - 1 + ny - 1 + nz - 1)

    def meta(h, to, at):
        return pltpu.make_async_remote_copy(
            src_ref=tv.at[h, to], dst_ref=trecv.at[h, mine[h]],
            send_sem=t_send.at[h * 4 + to], recv_sem=t_recv.at[h * 4 + at],
            device_id=peer(h, to), device_id_type=MESH)

    def early_copy(c, to, source):
        return pltpu.make_async_remote_copy(
            src_ref=early.at[c % PBUFS, to], dst_ref=x_early.at[c % RING, source],
            send_sem=e_send.at[c % PBUFS * groups + to],
            recv_sem=e_recv.at[c % RING * groups + source],
            device_id={"tau": to}, device_id_type=MESH)

    def late_copy(c, dest, source):
        return pltpu.make_async_remote_copy(
            src_ref=late.at[c, dest], dst_ref=x_late.at[c, source],
            send_sem=l_send.at[c * nx + dest],
            recv_sem=l_recv.at[c * groups + source],
            device_id={"tau": 2 * dest + 1}, device_id_type=MESH)

    def late_each(c, act):
        for step in range(nx):
            dest = (x + step) % nx
            if step == 0:
                @pl.when(core == 0)
                def _():
                    act(late_copy(c, dest, tau))
            else:
                act(late_copy(c, dest, tau))

    def y_copy(q, c, h, to, source):
        return pltpu.make_async_remote_copy(
            src_ref=ybuf.at[q, c % YBUFS, h, to], dst_ref=yrecv.at[q, c % RING, h, source],
            send_sem=y_send.at[((q * YBUFS + c % YBUFS) * 2 + h) * 4 + to],
            recv_sem=y_recv.at[((q * RING + c % RING) * 2 + h) * 4 + source],
            device_id=peer(h, to), device_id_type=MESH)

    def z_copy(q, h, to, source):
        return pltpu.make_async_remote_copy(
            src_ref=dense.at[q, h, to], dst_ref=zrecv.at[q, h, source],
            send_sem=z_send.at[(q * 2 + h) * 4 + to],
            recv_sem=z_recv.at[(q * 2 + h) * 4 + source],
            device_id=peer(1 - h, to), device_id_type=MESH)

    def back_copy(dest, source):
        return pltpu.make_async_remote_copy(
            src_ref=final.at[dest], dst_ref=back.at[source],
            send_sem=b_send.at[dest], recv_sem=b_recv.at[source],
            device_id={"tau": 2 * dest}, device_id_type=MESH)

    def back_each(act):
        for step in range(nx):
            dest = (x + step) % nx
            if step == 0:
                @pl.when(core == 1)
                def _():
                    act(back_copy(dest, tau))
            else:
                act(back_copy(dest, tau))

    for h in range(2):
        for to in others(h):
            meta(h, to, mine[h]).start()
        trecv[h, mine[h]] = tv[h, mine[h]]
        for s in range(sizes[h]):
            work[h, s * (slots + 1) + slots] = jnp.zeros((half, low, width), jnp.float32)

    @pl.loop(0, CHI_DEV)
    def _(e):
        for q in range(3):
            for h in range(2):
                for o in range(sizes[1 - h]):
                    dense[q, h, o, e] = jnp.zeros((half, low, width), jnp.float32)

    def compute(c):
        slot = c % PBUFS

        def one(i, last):
            n = c * per + i
            p = part[n]
            left = [occ[occ_idx[p * terms + j]] for j in range(terms)]
            right = [virt[virt_idx[p * terms + j]] for j in range(terms)]
            acc = jnp.dot(
                jnp.concatenate(left, axis=1),
                jnp.concatenate(right, axis=0),
                preferred_element_type=jnp.float32,
            )
            acc = acc + jnp.where(keep[n] != 0, last, 0.0)
            for g in range(groups):
                early[slot, g, i] = acc[g * rows:g * rows + low]
                upper = acc[g * rows + low:(g + 1) * rows]
                if g % 2 == 0:
                    timed[i, g // 2] = upper
                else:
                    late[c, g // 2, i] = upper
            return acc

        lax.fori_loop(0, per, one, jnp.zeros((rows * groups, width), jnp.float32),
                      unroll=math.gcd(per, 4))

    def transform(landed, at):
        @pl.loop(0, per, unroll=2)
        def _(i):
            values = [landed[at, s, i] for s in range(groups)]
            for k in range(freqs):
                total = weights[k, 0] * values[0]
                for s in range(1, groups):
                    total += weights[k, s] * values[s]
                freq[i, k] = total

    def send_y(q, c, values):
        @pl.when(c >= YBUFS)
        def _():
            for h in range(2):
                for to in others(h):
                    y_copy(q, c - YBUFS, h, to, mine[h]).wait_send()

        @pl.loop(0, nz)
        def _(dz):
            for dy in range(ny):
                for m in range(each):
                    i = place[(c * ny * nz + dz * ny + dy) * each + m]
                    ybuf[q, c % YBUFS, 0, dy, dz * each + m] = values[i, 0:half]
                    ybuf[q, c % YBUFS, 1, dz, dy * each + m] = values[i, half:freqs]

        for h in range(2):
            for to in others(h):
                y_copy(q, c, h, to, mine[h]).start()
            for e in range(slots):
                yrecv[q, c % RING, h, mine[h], e] = ybuf[q, c % YBUFS, h, mine[h], e]

    def tables():
        lane = lax.broadcasted_iota(jnp.int32, (CHUNKS, width), 1)
        for h in range(2):
            for s in others(h):
                meta(h, s, s).wait_recv()
            packed = jnp.zeros((CHUNKS, width), jnp.int32)
            for s in range(sizes[h]):
                found = jnp.full((CHUNKS, width), slots, jnp.int32)
                for e in range(slots):
                    found = jnp.where(trecv[h, s, e] == lane, e, found)
                packed = packed + (found + s * (slots + 1)) * (1 << (8 * s))
            tbl_v[h] = packed
        copy = pltpu.make_async_copy(tbl_v, tbl, tbl_sem)
        copy.start()
        copy.wait()

    def densify(q, c):
        for h in range(2):
            for s in others(h):
                y_copy(q, c, h, s, s).wait_recv()
            for s in range(sizes[h]):
                for e in range(slots):
                    work[h, s * (slots + 1) + e] = yrecv[q, c % RING, h, s, e]
        for h in range(2):
            @pl.loop(0, sizes[1 - h])
            def _(o):
                @pl.loop(0, CHI_DEV, unroll=8)
                def _(e):
                    packed = tbl[h, c, o * CHI_DEV + e]
                    total = dense[q, h, o, e]
                    for s in range(sizes[h]):
                        total += work[h, (packed >> (8 * s)) & 255]
                    dense[q, h, o, e] = total

    def send_z(q):
        for h in range(2):
            for to in others(1 - h):
                z_copy(q, h, to, mine[1 - h]).start()

    def finish(q, store):
        for h in range(2):
            for s in others(1 - h):
                z_copy(q, h, s, s).wait_recv()
            own = mine[1 - h]

            @pl.loop(0, CHI_DEV, unroll=4)
            def _(e):
                total = dense[q, h, own, e]
                for s in others(1 - h):
                    total += zrecv[q, h, s, e]
                for k in range(half):
                    store(h * half + k, e, total[k])

    def store_early(k, e, value):
        out[k, e, 0:low] = value

    def store_late(k, e, value):
        out[k, e, low:rows] = value

    def store_final(k, e, value):
        final[k, e] = value

    @pl.loop(0, rounds + LAG + 2)
    def _(t):
        @pl.when(t < rounds)
        def _():
            @pl.when(t >= PBUFS)
            def _():
                for to in times():
                    early_copy(t - PBUFS, to, tau).wait_send()
            compute(t)
            for to in times():
                early_copy(t, to, tau).start()

        @pl.when((t >= LAG) & (t < rounds + LAG))
        def _():
            late_each(t - LAG, lambda copy: copy.start())

        @pl.when(t < rounds)
        def _():
            send_y(2, t, timed)

            @pl.loop(0, per, unroll=4)
            def _(i):
                x_early[t % RING, tau, i] = early[t % PBUFS, tau, i]

        @pl.when((t >= 1) & (t < rounds + 1))
        def _():
            c = t - 1
            for s in times():
                early_copy(c, s, s).wait_recv()
            transform(x_early, c % RING)
            send_y(0, c, freq)

        @pl.when((t >= LAG + 1) & (t < rounds + LAG + 1) & (core == 1))
        def _():
            c = t - LAG - 1

            @pl.loop(0, per, unroll=4)
            def _(i):
                x_late[c, tau, i] = late[c, x, i]
            for s in times():
                late_copy(c, x, s).wait_recv()
            transform(x_late, c)
            send_y(1, c, freq)

        @pl.when(t == 1)
        def _():
            tables()

        @pl.when((t >= 1) & (t < rounds + 1))
        def _():
            densify(2, t - 1)

        @pl.when(t == rounds)
        def _():
            send_z(2)

        @pl.when((t >= 2) & (t < rounds + 2))
        def _():
            densify(0, t - 2)

        @pl.when(t == rounds + 1)
        def _():
            send_z(0)
            finish(2, store_final)
            back_each(lambda copy: copy.start())

        @pl.when((t >= LAG + 2) & (core == 1))
        def _():
            densify(1, t - LAG - 2)

    @pl.when(core == 1)
    def _():
        send_z(1)

    finish(0, store_early)

    @pl.when(core == 1)
    def _():
        finish(1, store_late)

    @pl.when(core == 0)
    def _():
        @pl.loop(0, CHI_DEV, unroll=4)
        def _(e):
            back[tau, e] = final[x, e]
        for s in times():
            back_copy(x, s).wait_recv()

        @pl.loop(0, CHI_DEV, unroll=2)
        def _(e):
            values = [back[s, e] for s in range(groups)]
            for k in range(freqs):
                total = weights[k, 0] * values[0]
                for s in range(1, groups):
                    total += weights[k, s] * values[s]
                out[k, e, low:rows] = total

    def drain(q):
        for h in range(2):
            for to in others(1 - h):
                z_copy(q, h, to, mine[1 - h]).wait_send()
            for c in range(rounds - YBUFS, rounds):
                for to in others(h):
                    y_copy(q, c, h, to, mine[h]).wait_send()

    for h in range(2):
        for to in others(h):
            meta(h, to, mine[h]).wait_send()
    drain(2)
    drain(0)
    pl.when(core == 1)(lambda: drain(1))
    back_each(lambda copy: copy.wait_send())

    @pl.loop(0, rounds)
    def _(c):
        late_each(c, lambda copy: copy.wait_send())

    @pl.loop(rounds - PBUFS, rounds)
    def _(c):
        for to in times():
            early_copy(c, to, tau).wait_send()


def plan(target, owners, ny, nz):
    count = target.shape[0]
    per = count // CHUNKS
    each = CAP // CHUNKS
    index = jnp.arange(count, dtype=jnp.int32)
    key = target * 256 + index
    rank = jnp.sum((key[None, :] < key[:, None]).astype(jnp.int32), axis=1)
    ordered = jnp.sum(jnp.where(rank[:, None] == index[None, :], key[:, None], 0), axis=0)
    ordered = ordered.reshape(per, CHUNKS).T
    part = ordered & 255
    tile = ordered >> 8
    same = (tile[:, 1:] == tile[:, :-1]).astype(jnp.int32)
    none = jnp.zeros((CHUNKS, 1), jnp.int32)
    keep = jnp.concatenate([none, same], axis=1)
    last = 1 - jnp.concatenate([same, none], axis=1)
    owner = tile // CHI_DEV
    value = jnp.where(last != 0, tile - owner * CHI_DEV, -1)
    d = jnp.arange(owners, dtype=jnp.int32)
    start = jnp.sum((owner[:, None, :] < d[None, :, None]).astype(jnp.int32), axis=2)
    place = start[:, :, None] + jnp.arange(each, dtype=jnp.int32)
    within = jnp.arange(per, dtype=jnp.int32)
    hit = (place[..., None] == within) & (owner[:, None, None, :] == d[None, :, None, None])
    goal = jnp.sum(jnp.where(hit, value[:, None, None, :] + 1, 0), axis=3) - 1
    place = jnp.minimum(place, per - 1)
    goal = goal.reshape(CHUNKS, nz, ny, each)
    zs = jnp.arange(nz, dtype=jnp.int32)[None, :, None, None] * CHI_DEV
    ys = jnp.arange(ny, dtype=jnp.int32)[None, None, :, None] * CHI_DEV
    to_y = jnp.where(goal >= 0, goal + zs, -1).transpose(2, 1, 3, 0).reshape(ny, nz * each, CHUNKS)
    to_z = jnp.where(goal >= 0, goal + ys, -1).transpose(1, 2, 3, 0).reshape(nz, ny * each, CHUNKS)
    both = jnp.stack([to_y, to_z])
    both = jnp.broadcast_to(both[..., None], both.shape + (128,))
    return part.reshape(-1), keep.reshape(-1), place.reshape(-1), both


def body(occupied, virtual, cos_weights, pair_occ, pair_virt, partial_target_tile):
    owners = lax.axis_size("tile")
    groups = lax.axis_size("tau")
    size = occupied.shape[2]
    terms = pair_occ.shape[1]
    count = partial_target_tile.shape[0]
    freqs = cos_weights.shape[0]
    ny = 1
    while 2 * ny * 2 * ny <= owners:
        ny *= 2
    nz = owners // ny
    rows = size // groups
    per = count // CHUNKS
    slots = ny * (CAP // CHUNKS)
    half = freqs // 2
    low = rows // 2
    nx = groups // 2
    part, keep, place, both = plan(partial_target_tile, owners, ny, nz)
    smem = pl.BlockSpec(memory_space=pltpu.SMEM)
    vmem = pl.BlockSpec(memory_space=pltpu.VMEM)
    dma = pltpu.SemaphoreType.DMA
    f32 = jnp.float32
    return pl.pallas_call(
        functools.partial(main_kernel, ny, nz, groups, terms),
        out_shape=jax.ShapeDtypeStruct((freqs, CHI_DEV, rows, size), f32),
        in_specs=[smem] * 6 + [vmem] * 3,
        out_specs=vmem,
        scratch_shapes=[
            pltpu.VMEM((PBUFS, groups, per, low, size), f32),
            pltpu.VMEM((CHUNKS, nx, per, low, size), f32),
            pltpu.VMEM((per, nx, low, size), f32),
            pltpu.VMEM((RING, groups, per, low, size), f32),
            pltpu.VMEM((CHUNKS, groups, per, low, size), f32),
            pltpu.VMEM((per, freqs, low, size), f32),
            pltpu.VMEM((3, YBUFS, 2, ny, slots, half, low, size), f32),
            pltpu.VMEM((3, RING, 2, ny, slots, half, low, size), f32),
            pltpu.VMEM((2, ny * (slots + 1), half, low, size), f32),
            pltpu.VMEM((3, 2, ny, CHI_DEV, half, low, size), f32),
            pltpu.VMEM((3, 2, ny, CHI_DEV, half, low, size), f32),
            pltpu.VMEM((nx, CHI_DEV, low, size), f32),
            pltpu.VMEM((groups, CHI_DEV, low, size), f32),
            pltpu.VMEM((2, ny, slots, CHUNKS, size), jnp.int32),
            pltpu.VMEM((2, CHUNKS, size), jnp.int32),
            pltpu.SMEM((2, CHUNKS, size), jnp.int32),
            dma((PBUFS * groups,)),
            dma((RING * groups,)),
            dma((CHUNKS * nx,)),
            dma((CHUNKS * groups,)),
            dma((3 * YBUFS * 8,)),
            dma((3 * RING * 8,)),
            dma((3 * 8,)),
            dma((3 * 8,)),
            dma((nx,)),
            dma((groups,)),
            dma((8,)),
            dma((8,)),
            dma,
        ],
        compiler_params=pltpu.CompilerParams(
            collective_id=0, has_side_effects=True, vmem_limit_bytes=62 * 1024 * 1024),
    )(cos_weights, pair_occ.reshape(-1), pair_virt.reshape(-1), part, keep, place,
      occupied[0], virtual[0], both)


def solution(mesh):
    in_specs = (
        P("tau", "tile", None, None),
        P("tau", "tile", None, None),
        P(),
        P("tile", None),
        P("tile", None),
        P("tile"),
    )
    out_specs = P(None, "tile", "tau", None)
    return jax.shard_map(body, mesh=mesh, in_specs=in_specs, out_specs=out_specs, check_vma=False)
```

```python
import functools
import math

import jax
import jax.numpy as jnp
from jax import lax
from jax.experimental import pallas as pl
from jax.experimental.pallas import tpu as pltpu
from jax.sharding import PartitionSpec as P

CHI_DEV = 32
CAP = 24
CHUNKS = 8
PBUFS = 4
YBUFS = 2
RING = 4
GROUP = 4
MESH = pl.DeviceIdType.MESH


def main_kernel(ny, nz, groups, terms,
                weights, occ_idx, virt_idx, part, keep, place, occ, virt, tv,
                out,
                early, late, timed, x_early, x_late, freq, ybuf, yrecv, work, scan, dense, zrecv,
                final, back, trecv, order_v, spot_v, order, spot,
                e_send, e_recv, l_send, l_recv, y_send, y_recv, z_send, z_recv,
                b_send, b_recv, t_send, t_recv, tbl_sem):
    tau = lax.axis_index("tau")
    tile = lax.axis_index("tile")
    x, core = tau // 2, tau % 2
    nx = groups // 2
    z, y = tile // ny, tile % ny
    mine = (y, z)
    sizes = (ny, nz)
    freqs, _, rows, width = out.shape
    low = rows // 2
    half = freqs // 2
    per = freq.shape[0]
    slots = yrecv.shape[4]
    each = slots // ny
    rounds = CHUNKS
    span = work.shape[2]
    share = slots * GROUP

    def peer(h, i):
        return {"tile": z * ny + i if h == 0 else i * ny + y}

    def others(h):
        return [(mine[h] + step) % sizes[h] for step in range(1, sizes[h])]

    def times():
        return [(tau + step) % groups for step in range(1, groups)]

    barrier = pltpu.get_barrier_semaphore()
    for to in times():
        pl.semaphore_signal(barrier, inc=1, device_id={"tau": to}, device_id_type=MESH)
    for h in range(2):
        for to in others(h):
            pl.semaphore_signal(barrier, inc=1, device_id=peer(h, to), device_id_type=MESH)
    pl.semaphore_wait(barrier, groups - 1 + ny - 1 + nz - 1)

    def meta(h, to, at):
        return pltpu.make_async_remote_copy(
            src_ref=tv.at[h * 4 + to], dst_ref=trecv.at[h * 4 + mine[h]],
            send_sem=t_send.at[h * 4 + to], recv_sem=t_recv.at[h * 4 + at],
            device_id=peer(h, to), device_id_type=MESH)

    def early_copy(c, to, source):
        return pltpu.make_async_remote_copy(
            src_ref=early.at[c % PBUFS, to], dst_ref=x_early.at[c, source],
            send_sem=e_send.at[c % PBUFS * groups + to],
            recv_sem=e_recv.at[c * groups + source],
            device_id={"tau": to}, device_id_type=MESH)

    def late_copy(c, dest, source):
        return pltpu.make_async_remote_copy(
            src_ref=late.at[c, dest], dst_ref=x_late.at[c, source],
            send_sem=l_send.at[c * nx + dest],
            recv_sem=l_recv.at[c * groups + source],
            device_id={"tau": 2 * dest + 1}, device_id_type=MESH)

    def late_each(c, act):
        for step in range(nx):
            dest = (x + step) % nx
            if step == 0:
                @pl.when(core == 0)
                def _():
                    act(late_copy(c, dest, tau))
            else:
                act(late_copy(c, dest, tau))

    def y_copy(q, n, h, to, source):
        return pltpu.make_async_remote_copy(
            src_ref=ybuf.at[q, n % YBUFS, h, to], dst_ref=yrecv.at[q, n % RING, h, source],
            send_sem=y_send.at[((q * YBUFS + n % YBUFS) * 2 + h) * 4 + to],
            recv_sem=y_recv.at[((q * RING + n % RING) * 2 + h) * 4 + source],
            device_id=peer(h, to), device_id_type=MESH)

    def z_copy(q, h, to, source):
        return pltpu.make_async_remote_copy(
            src_ref=dense.at[q, h, to], dst_ref=zrecv.at[q, h, source],
            send_sem=z_send.at[(q * 2 + h) * 4 + to],
            recv_sem=z_recv.at[(q * 2 + h) * 4 + source],
            device_id=peer(1 - h, to), device_id_type=MESH)

    def back_copy(dest, source):
        return pltpu.make_async_remote_copy(
            src_ref=final.at[dest], dst_ref=back.at[source],
            send_sem=b_send.at[dest], recv_sem=b_recv.at[source],
            device_id={"tau": 2 * dest}, device_id_type=MESH)

    def back_each(act):
        for step in range(nx):
            dest = (x + step) % nx
            if step == 0:
                @pl.when(core == 1)
                def _():
                    act(back_copy(dest, tau))
            else:
                act(back_copy(dest, tau))

    for h in range(2):
        for to in others(h):
            meta(h, to, mine[h]).start()
        trecv[h * 4 + mine[h]] = tv[h * 4 + mine[h]]
    scan[span] = jnp.zeros((half, low, width), jnp.float32)

    def compute(c):
        slot = c % PBUFS

        def one(i, last):
            p = part[c, i]
            left = [occ[occ_idx[j, p]] for j in range(terms)]
            right = [virt[virt_idx[j, p]] for j in range(terms)]
            acc = jnp.dot(
                jnp.concatenate(left, axis=1),
                jnp.concatenate(right, axis=0),
                preferred_element_type=jnp.float32,
            )
            acc = acc + jnp.where(keep[c, i] != 0, last, 0.0)
            for g in range(groups):
                early[slot, g, i] = acc[g * rows:g * rows + low]
                upper = acc[g * rows + low:(g + 1) * rows]
                if g % 2 == 0:
                    timed[i, g // 2] = upper
                else:
                    late[c, g // 2, i] = upper
            return acc

        lax.fori_loop(0, per, one, jnp.zeros((rows * groups, width), jnp.float32),
                      unroll=math.gcd(per, 4))

    def transform(landed, at):
        @pl.loop(0, per, unroll=2)
        def _(i):
            values = [landed[at, s, i] for s in range(groups)]
            for k in range(freqs):
                total = weights[k, 0] * values[0]
                for s in range(1, groups):
                    total += weights[k, s] * values[s]
                freq[i, k] = total

    def send_y(q, n, c, values):
        @pl.when(n >= YBUFS)
        def _():
            for h in range(2):
                for to in others(h):
                    y_copy(q, n - YBUFS, h, to, mine[h]).wait_send()

        @pl.loop(0, nz)
        def _(dz):
            for dy in range(ny):
                for m in range(each):
                    i = place[c, (dz * ny + dy) * each + m]
                    ybuf[q, n % YBUFS, 0, dy, dz * each + m] = values[i, 0:half]
                    ybuf[q, n % YBUFS, 1, dz, dy * each + m] = values[i, half:freqs]

        for h in range(2):
            for to in others(h):
                y_copy(q, n, h, to, mine[h]).start()
            for e in range(slots):
                yrecv[q, n % RING, h, mine[h], e] = ybuf[q, n % YBUFS, h, mine[h], e]

    def tables():
        for h in range(2):
            for s in others(h):
                meta(h, s, s).wait_recv()
            for g in range(CHUNKS // GROUP):
                lane = lax.broadcasted_iota(jnp.int32, (share, width), 1)
                local = lax.broadcasted_iota(jnp.int32, (share, width), 0)
                goal = jnp.concatenate([
                    jnp.sum(jnp.where(lane == local + g * share, trecv[h * 4 + s][0:1], 0),
                            axis=1, keepdims=True) for s in range(sizes[h])], axis=0)
                index = lax.broadcasted_iota(jnp.int32, (span, 1), 0)
                valid = goal >= 0
                goal = jnp.where(valid, goal, 200)
                column = goal * 256 + index
                wide = (span, 2 * width)
                across = lax.broadcasted_iota(jnp.int32, wide, 1)
                down = lax.broadcasted_iota(jnp.int32, wide, 0)
                column_w = jnp.broadcast_to(column, wide)
                goal_w = jnp.broadcast_to(goal, wide)
                row = jnp.sum(jnp.where(across == down, column_w, 0), axis=0, keepdims=True)
                row_goal = jnp.sum(jnp.where(across == down, goal_w, 0), axis=0, keepdims=True)
                before = (row < column_w) & (across < span)
                rank = jnp.sum(jnp.where(before, 1, 0), axis=1, keepdims=True)
                joined = jnp.max(jnp.where(before & (row_goal == goal_w), 1, 0),
                                 axis=1, keepdims=True)
                entry = index + 1024 * joined
                entry = jnp.sum(jnp.where(rank == across, entry, 0), axis=0, keepdims=True)
                at = h * (CHUNKS // GROUP) + g
                order_v[at:at + 1] = entry
                found = jnp.where((goal == across[:, :width]) & valid, rank, -1)
                found = jnp.max(found, axis=0, keepdims=True)
                found = jnp.where(found < 0, span, found)
                spot_v[at:at + 1] = found
        for i, (source, into) in enumerate(((order_v, order), (spot_v, spot))):
            copy = pltpu.make_async_copy(source, into, tbl_sem.at[i])
            copy.start()
            copy.wait()

    def collect(q, n):
        for h in range(2):
            for s in others(h):
                y_copy(q, n, h, s, s).wait_recv()
            for s in range(sizes[h]):
                for e in range(slots):
                    work[q, h, s * share + e * GROUP + n % GROUP] = yrecv[q, n % RING, h, s, e]

    def densify(q, stream, g):
        for h in range(2):
            at = h * (CHUNKS // GROUP) + g

            def one(r, last):
                entry = order[at, r]
                value = work[q, h, entry & 1023]
                value = value + jnp.where(entry >= 1024, last, 0.0)
                scan[r] = value
                return value

            lax.fori_loop(0, span, one, jnp.zeros((half, low, width), jnp.float32), unroll=8)

            @pl.loop(0, sizes[1 - h])
            def _(o):
                @pl.loop(0, CHI_DEV, unroll=8)
                def _(e):
                    value = scan[spot[at, o * CHI_DEV + e]]
                    if g:
                        value = value + dense[stream, h, o, e]
                    dense[stream, h, o, e] = value

    def send_z(q):
        for h in range(2):
            for to in others(1 - h):
                z_copy(q, h, to, mine[1 - h]).start()

    def finish(q, store):
        for h in range(2):
            for s in others(1 - h):
                z_copy(q, h, s, s).wait_recv()
            own = mine[1 - h]

            @pl.loop(0, CHI_DEV, unroll=4)
            def _(e):
                total = dense[q, h, own, e]
                for s in others(1 - h):
                    total += zrecv[q, h, s, e]
                for k in range(half):
                    store(h * half + k, e, total[k])

    def store_early(k, e, value):
        out[k, e, 0:low] = value

    def store_late(k, e, value):
        out[k, e, low:rows] = value

    def store_final(k, e, value):
        final[k, e] = value

    def when(condition):
        return pl.when(condition)

    @pl.loop(0, 2 * rounds + 3)
    def _(t):
        @when(t < rounds)
        def _():
            @when(t >= PBUFS)
            def _():
                for to in times():
                    early_copy(t - PBUFS, to, tau).wait_send()
            compute(t)
            for to in times():
                early_copy(t, to, tau).start()

        @when(t == rounds - 1)
        def _():
            @pl.loop(0, rounds)
            def _(c):
                late_each(c, lambda copy: copy.start())

        @when(t < rounds)
        def _():
            send_y(1, t, t, timed)

            @pl.loop(0, per, unroll=4)
            def _(i):
                x_early[t, tau, i] = early[t % PBUFS, tau, i]

        @when((t >= 2) & (t < rounds + 2))
        def _():
            c = t - 2
            for s in times():
                early_copy(c, s, s).wait_recv()
            transform(x_early, c)
            send_y(0, c, c, freq)

        @when((t >= rounds + 2) & (t < 2 * rounds + 2) & (core == 1))
        def _():
            c = t - rounds - 2

            @pl.loop(0, per, unroll=4)
            def _(i):
                x_late[c, tau, i] = late[c, x, i]
            for s in times():
                late_copy(c, x, s).wait_recv()
            transform(x_late, c)
            send_y(1, c + rounds, c, freq)

        @when(t == 1)
        def _():
            tables()

        @when((t >= 1) & (t < rounds + 1))
        def _():
            collect(1, t - 1)

        @when(t == GROUP)
        def _():
            densify(1, 2, 0)

        @when(t == rounds)
        def _():
            densify(1, 2, 1)
            send_z(2)

        @when((t >= 3) & (t < rounds + 3))
        def _():
            collect(0, t - 3)

        @when(t == GROUP + 2)
        def _():
            densify(0, 0, 0)

        @when(t == rounds + 2)
        def _():
            densify(0, 0, 1)
            send_z(0)

        @when(t == rounds + 3)
        def _():
            finish(2, store_final)
            back_each(lambda copy: copy.start())

        @when((t >= rounds + 3) & (core == 1))
        def _():
            collect(1, t - 3)

        @when((t == rounds + 2 + GROUP) & (core == 1))
        def _():
            densify(1, 1, 0)

        @when(t == rounds + 3 + GROUP)
        def _():
            finish(0, store_early)

    @when(core == 1)
    def _():
        densify(1, 1, 1)
        send_z(1)
        finish(1, store_late)

    @when(core == 0)
    def _():
        @pl.loop(0, CHI_DEV, unroll=4)
        def _(e):
            back[tau, e] = final[x, e]
        for s in times():
            back_copy(x, s).wait_recv()

        @pl.loop(0, CHI_DEV, unroll=2)
        def _(e):
            values = [back[s, e] for s in range(groups)]
            for k in range(freqs):
                total = weights[k, 0] * values[0]
                for s in range(1, groups):
                    total += weights[k, s] * values[s]
                out[k, e, low:rows] = total

    def drain_z(q):
        for h in range(2):
            for to in others(1 - h):
                z_copy(q, h, to, mine[1 - h]).wait_send()

    def drain_y(q):
        for h in range(2):
            for n in range(YBUFS):
                for to in others(h):
                    y_copy(q, n, h, to, mine[h]).wait_send()

    for h in range(2):
        for to in others(h):
            meta(h, to, mine[h]).wait_send()
    drain_z(2)
    drain_z(0)
    drain_y(0)
    drain_y(1)
    pl.when(core == 1)(lambda: drain_z(1))
    back_each(lambda copy: copy.wait_send())

    @pl.loop(0, rounds)
    def _(c):
        late_each(c, lambda copy: copy.wait_send())

    @pl.loop(rounds - PBUFS, rounds)
    def _(c):
        for to in times():
            early_copy(c, to, tau).wait_send()


def plan(target, owners, ny, nz):
    count = target.shape[0]
    per = count // CHUNKS
    each = CAP // CHUNKS
    index = jnp.arange(count, dtype=jnp.int32)
    key = target * 256 + index
    rank = jnp.sum((key[None, :] < key[:, None]).astype(jnp.int32), axis=1)
    at = jnp.arange(per)[None, :] * CHUNKS + jnp.arange(CHUNKS)[:, None]
    ordered = jnp.sum(jnp.where(rank == at[..., None], key, 0), axis=2)
    part = ordered & 255
    tile = ordered >> 8
    same = (tile[:, 1:] == tile[:, :-1]).astype(jnp.int32)
    none = jnp.zeros((CHUNKS, 1), jnp.int32)
    keep = jnp.concatenate([none, same], axis=1)
    last = 1 - jnp.concatenate([same, none], axis=1)
    owner = tile // CHI_DEV
    value = jnp.where(last != 0, tile - owner * CHI_DEV, -1)
    j = jnp.arange(owners * each, dtype=jnp.int32)
    d, m = j // each, j % each
    place = jnp.sum((owner[:, None, :] < d[None, :, None]).astype(jnp.int32), axis=2) + m
    within = jnp.arange(per, dtype=jnp.int32)
    hit = (place[..., None] == within) & (owner[:, None, :] == d[None, :, None])
    goal = jnp.sum(jnp.where(hit, value[:, None, :] + 1, 0), axis=2) - 1
    place = jnp.minimum(place, per - 1)
    goal = goal.reshape(CHUNKS // GROUP, GROUP, nz, ny, each)
    zs = jnp.arange(nz, dtype=jnp.int32)[:, None, None] * CHI_DEV
    ys = jnp.arange(ny, dtype=jnp.int32)[None, :, None] * CHI_DEV
    to_y = jnp.where(goal >= 0, goal + zs, -1).transpose(3, 0, 2, 4, 1).reshape(ny, -1)
    to_z = jnp.where(goal >= 0, goal + ys, -1).transpose(2, 0, 3, 4, 1).reshape(nz, -1)
    both = jnp.concatenate([to_y, to_z])
    both = jnp.pad(both, ((0, 0), (0, 128 - both.shape[1])))
    both = jnp.broadcast_to(both[:, None], (both.shape[0], 8, 128))
    return part, keep, place, both


def body(occupied, virtual, cos_weights, pair_occ, pair_virt, partial_target_tile):
    owners = lax.axis_size("tile")
    groups = lax.axis_size("tau")
    size = occupied.shape[2]
    terms = pair_occ.shape[1]
    count = partial_target_tile.shape[0]
    freqs = cos_weights.shape[0]
    ny = 1
    while 2 * ny * 2 * ny <= owners:
        ny *= 2
    nz = owners // ny
    rows = size // groups
    per = count // CHUNKS
    slots = ny * (CAP // CHUNKS)
    half = freqs // 2
    low = rows // 2
    nx = groups // 2
    span = ny * slots * GROUP
    part, keep, place, both = plan(partial_target_tile, owners, ny, nz)
    smem = pl.BlockSpec(memory_space=pltpu.SMEM)
    vmem = pl.BlockSpec(memory_space=pltpu.VMEM)
    dma = pltpu.SemaphoreType.DMA
    f32 = jnp.float32
    return pl.pallas_call(
        functools.partial(main_kernel, ny, nz, groups, terms),
        out_shape=jax.ShapeDtypeStruct((freqs, CHI_DEV, rows, size), f32),
        in_specs=[smem] * 6 + [vmem] * 3,
        out_specs=vmem,
        scratch_shapes=[
            pltpu.VMEM((PBUFS, groups, per, low, size), f32),
            pltpu.VMEM((CHUNKS, nx, per, low, size), f32),
            pltpu.VMEM((per, nx, low, size), f32),
            pltpu.VMEM((CHUNKS, groups, per, low, size), f32),
            pltpu.VMEM((CHUNKS, groups, per, low, size), f32),
            pltpu.VMEM((per, freqs, low, size), f32),
            pltpu.VMEM((2, YBUFS, 2, ny, slots, half, low, size), f32),
            pltpu.VMEM((2, RING, 2, ny, slots, half, low, size), f32),
            pltpu.VMEM((2, 2, span, half, low, size), f32),
            pltpu.VMEM((span + 1, half, low, size), f32),
            pltpu.VMEM((3, 2, ny, CHI_DEV, half, low, size), f32),
            pltpu.VMEM((3, 2, ny, CHI_DEV, half, low, size), f32),
            pltpu.VMEM((nx, CHI_DEV, low, size), f32),
            pltpu.VMEM((groups, CHI_DEV, low, size), f32),
            pltpu.VMEM((8, 8, size), jnp.int32),
            pltpu.VMEM((8, 2 * size), jnp.int32),
            pltpu.VMEM((8, size), jnp.int32),
            pltpu.SMEM((8, 2 * size), jnp.int32),
            pltpu.SMEM((8, size), jnp.int32),
            dma((PBUFS * groups,)),
            dma((CHUNKS * groups,)),
            dma((CHUNKS * nx,)),
            dma((CHUNKS * groups,)),
            dma((2 * YBUFS * 8,)),
            dma((2 * RING * 8,)),
            dma((3 * 8,)),
            dma((3 * 8,)),
            dma((nx,)),
            dma((groups,)),
            dma((8,)),
            dma((8,)),
            dma((2,)),
        ],
        compiler_params=pltpu.CompilerParams(
            collective_id=0, has_side_effects=True, vmem_limit_bytes=62 * 1024 * 1024),
    )(cos_weights, pair_occ.T, pair_virt.T, part, keep, place,
      occupied[0], virtual[0], both)


def solution(mesh):
    in_specs = (
        P("tau", "tile", None, None),
        P("tau", "tile", None, None),
        P(),
        P("tile", None),
        P("tile", None),
        P("tile"),
    )
    out_specs = P(None, "tile", "tau", None)
    return jax.shard_map(body, mesh=mesh, in_specs=in_specs, out_specs=out_specs, check_vma=False)
```

```python
import functools
import math

import jax
import jax.numpy as jnp
from jax import lax
from jax.experimental import pallas as pl
from jax.experimental.pallas import tpu as pltpu
from jax.sharding import PartitionSpec as P

CHI_DEV = 32
CAP = 24
CHUNKS = 8
PBUFS = 4
YBUFS = (2, 4)
RINGS = (4, 8)
XRING = 6
PARTS = 2
GROUP = 4
LATER = 3
FSTEP = 5
LOADS = 4
MESH = pl.DeviceIdType.MESH


def main_kernel(ny, nz, groups, terms,
                weights_in, occ_idx_in, virt_idx_in, steps_in, tv_in, occ_hbm, virt_hbm,
                out,
                occ, virt, weights, occ_idx, virt_idx, steps, tv, early, late, timed, x_early, x_late, freq, y_out_first, y_out_second, y_first, y_second, work, scan, dense, zrecv,
                final, back, trecv, order_v, spot_v, order, spot,
                e_send, e_recv, l_send, l_recv, y_send, y_recv, z_send, z_recv,
                b_send, b_recv, t_send, t_recv, tbl_sem, load_sem):
    tau = lax.axis_index("tau")
    tile = lax.axis_index("tile")
    x, core = tau // 2, tau % 2
    nx = groups // 2
    z, y = tile // ny, tile % ny
    mine = (y, z)
    sizes = (ny, nz)
    freqs, _, rows, width = out.shape
    low = rows // 2
    half = freqs // 2
    per = freq.shape[0]
    slots = y_first.shape[3]
    each = slots // ny
    rounds = CHUNKS
    span = work.shape[2]
    share = slots * GROUP

    def peer(h, i):
        return {"tile": z * ny + i if h == 0 else i * ny + y}

    def others(h):
        return [(mine[h] + step) % sizes[h] for step in range(1, sizes[h])]

    def times():
        return [(tau + step) % groups for step in range(1, groups)]

    landing = (y_first, y_second)
    ring = (y_first.shape[0], y_second.shape[0])
    base = (0, ring[0])
    leaving = (y_out_first, y_out_second)
    outs = (y_out_first.shape[0], y_out_second.shape[0])
    out_base = (0, outs[0])
    part_size = occ.shape[0] // LOADS

    def load(i):
        at = pl.ds(i % LOADS * part_size, part_size)
        source, into = ((occ_hbm, occ), (virt_hbm, virt))[i // LOADS]
        return pltpu.make_async_copy(source.at[at], into.at[at], load_sem.at[i])

    small = [
        pltpu.make_async_copy(source, into, load_sem.at[2 * LOADS + i])
        for i, (source, into) in enumerate((
            (tv_in, tv), (occ_idx_in, occ_idx), (virt_idx_in, virt_idx),
            (steps_in, steps), (weights_in, weights)))
    ]
    for copy in small:
        copy.start()
    for i in range(2 * LOADS):
        load(i).start()

    barrier = pltpu.get_barrier_semaphore()
    for to in times():
        pl.semaphore_signal(barrier, inc=1, device_id={"tau": to}, device_id_type=MESH)
    for h in range(2):
        for to in others(h):
            pl.semaphore_signal(barrier, inc=1, device_id=peer(h, to), device_id_type=MESH)
    pl.semaphore_wait(barrier, groups - 1 + ny - 1 + nz - 1)

    def meta(h, to, at):
        return pltpu.make_async_remote_copy(
            src_ref=tv.at[h * 4 + to], dst_ref=trecv.at[h * 4 + mine[h]],
            send_sem=t_send.at[h * 4 + to], recv_sem=t_recv.at[h * 4 + at],
            device_id=peer(h, to), device_id_type=MESH)

    def early_copy(c, to, source, at=None):
        at = pl.ds(0, per) if at is None else at
        return pltpu.make_async_remote_copy(
            src_ref=early.at[c % PBUFS, to, at], dst_ref=x_early.at[c % XRING, source, at],
            send_sem=e_send.at[c % PBUFS * groups + to],
            recv_sem=e_recv.at[c % XRING * groups + source],
            device_id={"tau": to}, device_id_type=MESH)

    def late_copy(c, dest, source):
        return pltpu.make_async_remote_copy(
            src_ref=late.at[c, dest], dst_ref=x_late.at[c, source],
            send_sem=l_send.at[c * nx + dest],
            recv_sem=l_recv.at[c * groups + source],
            device_id={"tau": 2 * dest + 1}, device_id_type=MESH)

    def late_each(c, act):
        for step in range(nx):
            dest = (x + step) % nx
            if step == 0:
                @pl.when(core == 0)
                def _():
                    act(late_copy(c, dest, tau))
            else:
                act(late_copy(c, dest, tau))

    def y_copy(q, n, h, to, source):
        return pltpu.make_async_remote_copy(
            src_ref=leaving[q].at[n % outs[q], h, to], dst_ref=landing[q].at[n % ring[q], h, source],
            send_sem=y_send.at[((out_base[q] + n % outs[q]) * 2 + h) * 4 + to],
            recv_sem=y_recv.at[((base[q] + n % ring[q]) * 2 + h) * 4 + source],
            device_id=peer(h, to), device_id_type=MESH)

    def z_copy(q, h, to, source):
        return pltpu.make_async_remote_copy(
            src_ref=dense.at[q, h, to], dst_ref=zrecv.at[q, h, source],
            send_sem=z_send.at[(q * 2 + h) * 4 + to],
            recv_sem=z_recv.at[(q * 2 + h) * 4 + source],
            device_id=peer(1 - h, to), device_id_type=MESH)

    def back_copy(dest, source):
        return pltpu.make_async_remote_copy(
            src_ref=final.at[dest], dst_ref=back.at[source],
            send_sem=b_send.at[dest], recv_sem=b_recv.at[source],
            device_id={"tau": 2 * dest}, device_id_type=MESH)

    def back_each(act):
        for step in range(nx):
            dest = (x + step) % nx
            if step == 0:
                @pl.when(core == 1)
                def _():
                    act(back_copy(dest, tau))
            else:
                act(back_copy(dest, tau))

    for copy in small:
        copy.wait()
    for h in range(2):
        for to in others(h):
            meta(h, to, mine[h]).start()
        trecv[h * 4 + mine[h]] = tv[h * 4 + mine[h]]
    scan[span] = jnp.zeros((half, low, width), jnp.float32)
    for i in range(2 * LOADS):
        load(i).wait()

    def compute(c):
        slot = c % PBUFS

        def one(i, last):
            p = steps[c, i]
            left = [occ[occ_idx[j, p]] for j in range(terms)]
            right = [virt[virt_idx[j, p]] for j in range(terms)]
            acc = jnp.dot(
                jnp.concatenate(left, axis=1),
                jnp.concatenate(right, axis=0),
                preferred_element_type=jnp.float32,
            )
            acc = acc + jnp.where(steps[c, per + i] != 0, last, 0.0)
            for g in range(groups):
                early[slot, g, i] = acc[g * rows:g * rows + low]
                upper = acc[g * rows + low:(g + 1) * rows]
                if g % 2 == 0:
                    timed[i, g // 2] = upper
                else:
                    late[c, g // 2, i] = upper
            return acc

        size = per // PARTS

        def portion(k, last):
            last = lax.fori_loop(
                0, size, lambda i, last: one(k * size + i, last), last,
                unroll=math.gcd(size, 4))
            for to in times():
                early_copy(c, to, tau, pl.ds(k * size, size)).start()
            return last

        lax.fori_loop(0, PARTS, portion, jnp.zeros((rows * groups, width), jnp.float32))

    def transform(landed, at):
        @pl.loop(0, per, unroll=2)
        def _(i):
            values = [landed[at, s, i] for s in range(groups)]
            for k in range(freqs):
                total = weights[k, 0] * values[0]
                for s in range(1, groups):
                    total += weights[k, s] * values[s]
                freq[i, k] = total

    def send_y(q, n, c, values):
        @pl.when(n >= outs[q])
        def _():
            for h in range(2):
                for to in others(h):
                    y_copy(q, n - outs[q], h, to, mine[h]).wait_send()

        @pl.loop(0, nz)
        def _(dz):
            for dy in range(ny):
                for m in range(each):
                    i = steps[c, 2 * per + (dz * ny + dy) * each + m]
                    leaving[q][n % outs[q], 0, dy, dz * each + m] = values[i, 0:half]
                    leaving[q][n % outs[q], 1, dz, dy * each + m] = values[i, half:freqs]

        for h in range(2):
            for to in others(h):
                y_copy(q, n, h, to, mine[h]).start()
            for e in range(slots):
                landing[q][n % ring[q], h, mine[h], e] = leaving[q][n % outs[q], h, mine[h], e]

    def tables():
        for h in range(2):
            for s in others(h):
                meta(h, s, s).wait_recv()
            for g in range(CHUNKS // GROUP):
                lane = lax.broadcasted_iota(jnp.int32, (share, width), 1)
                local = lax.broadcasted_iota(jnp.int32, (share, width), 0)
                goal = jnp.concatenate([
                    jnp.sum(jnp.where(lane == local + g * share, trecv[h * 4 + s][0:1], 0),
                            axis=1, keepdims=True) for s in range(sizes[h])], axis=0)
                index = lax.broadcasted_iota(jnp.int32, (span, 1), 0)
                valid = goal >= 0
                goal = jnp.where(valid, goal, 200)
                column = goal * 256 + index
                wide = (span, 2 * width)
                across = lax.broadcasted_iota(jnp.int32, wide, 1)
                down = lax.broadcasted_iota(jnp.int32, wide, 0)
                column_w = jnp.broadcast_to(column, wide)
                goal_w = jnp.broadcast_to(goal, wide)
                row = jnp.sum(jnp.where(across == down, column_w, 0), axis=0, keepdims=True)
                row_goal = jnp.sum(jnp.where(across == down, goal_w, 0), axis=0, keepdims=True)
                before = (row < column_w) & (across < span)
                rank = jnp.sum(jnp.where(before, 1, 0), axis=1, keepdims=True)
                joined = jnp.max(jnp.where(before & (row_goal == goal_w), 1, 0),
                                 axis=1, keepdims=True)
                entry = index + 1024 * joined
                entry = jnp.sum(jnp.where(rank == across, entry, 0), axis=0, keepdims=True)
                at = h * (CHUNKS // GROUP) + g
                order_v[at:at + 1] = entry
                found = jnp.where((goal == across[:, :width]) & valid, rank, -1)
                found = jnp.max(found, axis=0, keepdims=True)
                found = jnp.where(found < 0, span, found)
                spot_v[at:at + 1] = found
        for i, (source, into) in enumerate(((order_v, order), (spot_v, spot))):
            copy = pltpu.make_async_copy(source, into, tbl_sem.at[i])
            copy.start()
            copy.wait()

    def collect(q, n):
        for h in range(2):
            for s in others(h):
                y_copy(q, n, h, s, s).wait_recv()
            for s in range(sizes[h]):
                for e in range(slots):
                    work[q, h, s * share + e * GROUP + n % GROUP] = landing[q][n % ring[q], h, s, e]

    def densify(q, stream, g):
        for h in range(2):
            at = h * (CHUNKS // GROUP) + g

            def one(r, last):
                entry = order[at, r]
                value = work[q, h, entry & 1023]
                value = value + jnp.where(entry >= 1024, last, 0.0)
                scan[r] = value
                return value

            lax.fori_loop(0, span, one, jnp.zeros((half, low, width), jnp.float32), unroll=8)

            @pl.loop(0, sizes[1 - h])
            def _(o):
                @pl.loop(0, CHI_DEV, unroll=8)
                def _(e):
                    value = scan[spot[at, o * CHI_DEV + e]]
                    if g:
                        value = value + dense[stream, h, o, e]
                    dense[stream, h, o, e] = value

    def send_z(q):
        for h in range(2):
            for to in others(1 - h):
                z_copy(q, h, to, mine[1 - h]).start()

    def finish(q, store):
        for h in range(2):
            for s in others(1 - h):
                z_copy(q, h, s, s).wait_recv()
            own = mine[1 - h]

            @pl.loop(0, CHI_DEV, unroll=4)
            def _(e):
                total = dense[q, h, own, e]
                for s in others(1 - h):
                    total += zrecv[q, h, s, e]
                for k in range(half):
                    store(h * half + k, e, total[k])

    def store_early(k, e, value):
        out[k, e, 0:low] = value

    def store_late(k, e, value):
        out[k, e, low:rows] = value

    def store_final(k, e, value):
        final[k, e] = value

    def when(condition):
        return pl.when(condition)

    @pl.loop(0, 2 * rounds + 2 + LATER)
    def _(t):
        @when(t < rounds)
        def _():
            @when(t >= PBUFS)
            def _():
                for to in times():
                    early_copy(t - PBUFS, to, tau).wait_send()
            compute(t)

        @when(t == rounds - 1)
        def _():
            @pl.loop(0, rounds)
            def _(c):
                late_each(c, lambda copy: copy.start())

        @when(t < rounds)
        def _():
            send_y(1, t, t, timed)

            @pl.loop(0, per, unroll=4)
            def _(i):
                x_early[t % XRING, tau, i] = early[t % PBUFS, tau, i]

        @when((t >= 2) & (t < rounds + 2))
        def _():
            c = t - 2
            for s in times():
                early_copy(c, s, s).wait_recv()
            transform(x_early, c % XRING)
            send_y(0, c, c, freq)

        @when((t >= rounds + 2) & (t < 2 * rounds + 2) & (core == 1))
        def _():
            c = t - rounds - 2

            @pl.loop(0, per, unroll=4)
            def _(i):
                x_late[c, tau, i] = late[c, x, i]
            for s in times():
                late_copy(c, x, s).wait_recv()
            transform(x_late, c)
            send_y(1, c + rounds, c, freq)

        @when(t == 1)
        def _():
            tables()

        @when((t >= 1) & (t < rounds + 1))
        def _():
            collect(1, t - 1)

        @when(t == GROUP)
        def _():
            densify(1, 2, 0)

        @when(t == rounds)
        def _():
            densify(1, 2, 1)

        @when((t >= 3) & (t < rounds + 1))
        def _():
            collect(0, t - 3)

        @when(t == GROUP + 2)
        def _():
            densify(0, 0, 0)

        @when(t == rounds + 1)
        def _():
            send_z(2)

        @when(t == rounds + 3)
        def _():
            collect(0, rounds - 2)
            collect(0, rounds - 1)
            densify(0, 0, 1)
            send_z(0)

        @when(t == rounds + FSTEP)
        def _():
            finish(2, store_final)
            back_each(lambda copy: copy.start())

        @when((t >= rounds + 2 + LATER) & (core == 1))
        def _():
            collect(1, t - 2 - LATER)

        @when((t == rounds + 1 + LATER + GROUP) & (core == 1))
        def _():
            densify(1, 1, 0)

    @when(core == 1)
    def _():
        densify(1, 1, 1)
        send_z(1)

    finish(0, store_early)

    @when(core == 1)
    def _():
        finish(1, store_late)

    @when(core == 0)
    def _():
        @pl.loop(0, CHI_DEV, unroll=4)
        def _(e):
            back[tau, e] = final[x, e]
        for s in times():
            back_copy(x, s).wait_recv()

        @pl.loop(0, CHI_DEV, unroll=2)
        def _(e):
            values = [back[s, e] for s in range(groups)]
            for k in range(freqs):
                total = weights[k, 0] * values[0]
                for s in range(1, groups):
                    total += weights[k, s] * values[s]
                out[k, e, low:rows] = total

    def drain_z(q):
        for h in range(2):
            for to in others(1 - h):
                z_copy(q, h, to, mine[1 - h]).wait_send()

    def drain_y(q):
        for h in range(2):
            for n in range(outs[q]):
                for to in others(h):
                    y_copy(q, n, h, to, mine[h]).wait_send()

    for h in range(2):
        for to in others(h):
            meta(h, to, mine[h]).wait_send()
    drain_z(2)
    drain_z(0)
    drain_y(0)
    drain_y(1)
    pl.when(core == 1)(lambda: drain_z(1))
    back_each(lambda copy: copy.wait_send())

    @pl.loop(0, rounds)
    def _(c):
        late_each(c, lambda copy: copy.wait_send())

    @pl.loop(rounds - PBUFS, rounds)
    def _(c):
        for to in times():
            early_copy(c, to, tau).wait_send()


def plan(target, owners, ny, nz):
    count = target.shape[0]
    per = count // CHUNKS
    each = CAP // CHUNKS
    index = jnp.arange(count, dtype=jnp.int32)
    key = target * 256 + index
    rank = jnp.sum((key[None, :] < key[:, None]).astype(jnp.int32), axis=1)
    at = jnp.arange(per)[None, :] * CHUNKS + jnp.arange(CHUNKS)[:, None]
    ordered = jnp.sum(jnp.where(rank == at[..., None], key, 0), axis=2)
    part = ordered & 255
    tile = ordered >> 8
    same = (tile[:, 1:] == tile[:, :-1]).astype(jnp.int32)
    none = jnp.zeros((CHUNKS, 1), jnp.int32)
    keep = jnp.concatenate([none, same], axis=1)
    last = 1 - jnp.concatenate([same, none], axis=1)
    owner = tile // CHI_DEV
    value = jnp.where(last != 0, tile - owner * CHI_DEV, -1)
    j = jnp.arange(owners * each, dtype=jnp.int32)
    d, m = j // each, j % each
    place = jnp.sum((owner[:, None, :] < d[None, :, None]).astype(jnp.int32), axis=2) + m
    within = jnp.arange(per, dtype=jnp.int32)
    hit = (place[..., None] == within) & (owner[:, None, :] == d[None, :, None])
    goal = jnp.sum(jnp.where(hit, value[:, None, :] + 1, 0), axis=2) - 1
    place = jnp.minimum(place, per - 1)
    goal = goal.reshape(CHUNKS // GROUP, GROUP, nz, ny, each)
    zs = jnp.arange(nz, dtype=jnp.int32)[:, None, None] * CHI_DEV
    ys = jnp.arange(ny, dtype=jnp.int32)[None, :, None] * CHI_DEV
    to_y = jnp.where(goal >= 0, goal + zs, -1).transpose(3, 0, 2, 4, 1).reshape(ny, -1)
    to_z = jnp.where(goal >= 0, goal + ys, -1).transpose(2, 0, 3, 4, 1).reshape(nz, -1)
    both = jnp.concatenate([to_y, to_z])
    both = jnp.pad(both, ((0, 0), (0, 128 - both.shape[1])))
    both = jnp.broadcast_to(both[:, None], (both.shape[0], 8, 128))
    return jnp.concatenate([part, keep, place], axis=1), both


def body(occupied, virtual, cos_weights, pair_occ, pair_virt, partial_target_tile):
    owners = lax.axis_size("tile")
    groups = lax.axis_size("tau")
    size = occupied.shape[2]
    terms = pair_occ.shape[1]
    count = partial_target_tile.shape[0]
    freqs = cos_weights.shape[0]
    ny = 1
    while 2 * ny * 2 * ny <= owners:
        ny *= 2
    nz = owners // ny
    rows = size // groups
    per = count // CHUNKS
    slots = ny * (CAP // CHUNKS)
    half = freqs // 2
    low = rows // 2
    nx = groups // 2
    span = ny * slots * GROUP
    steps, both = plan(partial_target_tile, owners, ny, nz)
    vmem = pl.BlockSpec(memory_space=pltpu.VMEM)
    dma = pltpu.SemaphoreType.DMA
    f32 = jnp.float32
    return pl.pallas_call(
        functools.partial(main_kernel, ny, nz, groups, terms),
        out_shape=jax.ShapeDtypeStruct((freqs, CHI_DEV, rows, size), f32),
        in_specs=[pl.BlockSpec(memory_space=pl.ANY)] * 7,
        out_specs=vmem,
        scratch_shapes=[
            pltpu.VMEM(occupied.shape[1:], occupied.dtype),
            pltpu.VMEM(virtual.shape[1:], virtual.dtype),
            pltpu.SMEM(cos_weights.shape, f32),
            pltpu.SMEM((terms, count), jnp.int32),
            pltpu.SMEM((terms, count), jnp.int32),
            pltpu.SMEM(steps.shape, jnp.int32),
            pltpu.VMEM(both.shape, jnp.int32),
            pltpu.VMEM((PBUFS, groups, per, low, size), f32),
            pltpu.VMEM((CHUNKS, nx, per, low, size), f32),
            pltpu.VMEM((per, nx, low, size), f32),
            pltpu.VMEM((XRING, groups, per, low, size), f32),
            pltpu.VMEM((CHUNKS, groups, per, low, size), f32),
            pltpu.VMEM((per, freqs, low, size), f32),
            pltpu.VMEM((YBUFS[0], 2, ny, slots, half, low, size), f32),
            pltpu.VMEM((YBUFS[1], 2, ny, slots, half, low, size), f32),
            pltpu.VMEM((RINGS[0], 2, ny, slots, half, low, size), f32),
            pltpu.VMEM((RINGS[1], 2, ny, slots, half, low, size), f32),
            pltpu.VMEM((2, 2, span, half, low, size), f32),
            pltpu.VMEM((span + 1, half, low, size), f32),
            pltpu.VMEM((3, 2, ny, CHI_DEV, half, low, size), f32),
            pltpu.VMEM((3, 2, ny, CHI_DEV, half, low, size), f32),
            pltpu.VMEM((nx, CHI_DEV, low, size), f32),
            pltpu.VMEM((groups, CHI_DEV, low, size), f32),
            pltpu.VMEM((8, 8, size), jnp.int32),
            pltpu.VMEM((8, 2 * size), jnp.int32),
            pltpu.VMEM((8, size), jnp.int32),
            pltpu.SMEM((8, 2 * size), jnp.int32),
            pltpu.SMEM((8, size), jnp.int32),
            dma((PBUFS * groups,)),
            dma((XRING * groups,)),
            dma((CHUNKS * nx,)),
            dma((CHUNKS * groups,)),
            dma((sum(YBUFS) * 8,)),
            dma((sum(RINGS) * 8,)),
            dma((3 * 8,)),
            dma((3 * 8,)),
            dma((nx,)),
            dma((groups,)),
            dma((8,)),
            dma((8,)),
            dma((2,)),
            dma((2 * LOADS + 5,)),
        ],
        compiler_params=pltpu.CompilerParams(
            collective_id=0, has_side_effects=True, vmem_limit_bytes=63 * 1024 * 1024),
    )(cos_weights, pair_occ.T, pair_virt.T, steps,
      both, occupied[0], virtual[0])


def solution(mesh):
    in_specs = (
        P("tau", "tile", None, None),
        P("tau", "tile", None, None),
        P(),
        P("tile", None),
        P("tile", None),
        P("tile"),
    )
    out_specs = P(None, "tile", "tau", None)
    return jax.shard_map(body, mesh=mesh, in_specs=in_specs, out_specs=out_specs, check_vma=False)
```

```python
import functools
import math

import jax
import jax.numpy as jnp
from jax import lax
from jax.experimental import pallas as pl
from jax.experimental.pallas import tpu as pltpu
from jax.sharding import PartitionSpec as P

CHI_DEV = 32
CAP = 24
CHUNKS = 8
PBUFS = 4
YBUFS = (2, 4)
RINGS = (6, 8)
XRING = 6
PARTS = 2
GROUP = 4
LATER = 8
FSTEP = 5
ZLATE = 9
LOADS = 4
MESH = pl.DeviceIdType.MESH


def main_kernel(ny, nz, groups, terms,
                weights_in, occ_idx_in, virt_idx_in, steps_in, tv_in, occ_hbm, virt_hbm,
                out,
                occ, virt, weights, occ_idx, virt_idx, steps, tv, early, late, timed, x_early, x_late, freq, y_out_first, y_out_second, y_first, y_second, work, scan, dense, zrecv,
                final, back, trecv, order_v, spot_v, order, spot,
                e_send, e_recv, l_send, l_recv, y_send, y_recv, z_send, z_recv,
                b_send, b_recv, t_send, t_recv, tbl_sem, load_sem):
    tau = lax.axis_index("tau")
    tile = lax.axis_index("tile")
    x, core = tau // 2, tau % 2
    nx = groups // 2
    z, y = tile // ny, tile % ny
    mine = (y, z)
    sizes = (ny, nz)
    freqs, _, rows, width = out.shape
    low = rows // 2
    half = freqs // 2
    per = freq.shape[0]
    slots = y_first.shape[3]
    each = slots // ny
    rounds = CHUNKS
    span = work.shape[2]
    share = slots * GROUP

    def peer(h, i):
        return {"tile": z * ny + i if h == 0 else i * ny + y}

    def others(h):
        return [(mine[h] + step) % sizes[h] for step in range(1, sizes[h])]

    def times():
        return [(tau + step) % groups for step in range(1, groups)]

    landing = (y_first, y_second)
    ring = (y_first.shape[0], y_second.shape[0])
    base = (0, ring[0])
    leaving = (y_out_first, y_out_second)
    outs = (y_out_first.shape[0], y_out_second.shape[0])
    out_base = (0, outs[0])
    part_size = occ.shape[0] // LOADS

    def load(i):
        at = pl.ds(i % LOADS * part_size, part_size)
        source, into = ((occ_hbm, occ), (virt_hbm, virt))[i // LOADS]
        return pltpu.make_async_copy(source.at[at], into.at[at], load_sem.at[i])

    small = [
        pltpu.make_async_copy(source, into, load_sem.at[2 * LOADS + i])
        for i, (source, into) in enumerate((
            (tv_in, tv), (occ_idx_in, occ_idx), (virt_idx_in, virt_idx),
            (steps_in, steps), (weights_in, weights)))
    ]
    for copy in small:
        copy.start()
    for i in range(2 * LOADS):
        load(i).start()

    barrier = pltpu.get_barrier_semaphore()
    for to in times():
        pl.semaphore_signal(barrier, inc=1, device_id={"tau": to}, device_id_type=MESH)
    for h in range(2):
        for to in others(h):
            pl.semaphore_signal(barrier, inc=1, device_id=peer(h, to), device_id_type=MESH)
    pl.semaphore_wait(barrier, groups - 1 + ny - 1 + nz - 1)

    def meta(h, to, at):
        return pltpu.make_async_remote_copy(
            src_ref=tv.at[h * 4 + to], dst_ref=trecv.at[h * 4 + mine[h]],
            send_sem=t_send.at[h * 4 + to], recv_sem=t_recv.at[h * 4 + at],
            device_id=peer(h, to), device_id_type=MESH)

    def early_copy(c, to, source, at=None):
        at = pl.ds(0, per) if at is None else at
        return pltpu.make_async_remote_copy(
            src_ref=early.at[c % PBUFS, to, at], dst_ref=x_early.at[c % XRING, source, at],
            send_sem=e_send.at[c % PBUFS * groups + to],
            recv_sem=e_recv.at[c % XRING * groups + source],
            device_id={"tau": to}, device_id_type=MESH)

    def late_copy(c, dest, source):
        return pltpu.make_async_remote_copy(
            src_ref=late.at[c, dest], dst_ref=x_late.at[c, source],
            send_sem=l_send.at[c * nx + dest],
            recv_sem=l_recv.at[c * groups + source],
            device_id={"tau": 2 * dest + 1}, device_id_type=MESH)

    def late_each(c, act):
        for step in range(nx):
            dest = (x + step) % nx
            if step == 0:
                @pl.when(core == 0)
                def _():
                    act(late_copy(c, dest, tau))
            else:
                act(late_copy(c, dest, tau))

    def y_copy(q, n, h, to, source):
        return pltpu.make_async_remote_copy(
            src_ref=leaving[q].at[n % outs[q], h, to], dst_ref=landing[q].at[n % ring[q], h, source],
            send_sem=y_send.at[((out_base[q] + n % outs[q]) * 2 + h) * 4 + to],
            recv_sem=y_recv.at[((base[q] + n % ring[q]) * 2 + h) * 4 + source],
            device_id=peer(h, to), device_id_type=MESH)

    def z_copy(q, h, to, source):
        return pltpu.make_async_remote_copy(
            src_ref=dense.at[q, h, to], dst_ref=zrecv.at[q, h, source],
            send_sem=z_send.at[(q * 2 + h) * 4 + to],
            recv_sem=z_recv.at[(q * 2 + h) * 4 + source],
            device_id=peer(1 - h, to), device_id_type=MESH)

    def back_copy(dest, source):
        return pltpu.make_async_remote_copy(
            src_ref=final.at[dest], dst_ref=back.at[source],
            send_sem=b_send.at[dest], recv_sem=b_recv.at[source],
            device_id={"tau": 2 * dest}, device_id_type=MESH)

    def back_each(act):
        for step in range(nx):
            dest = (x + step) % nx
            if step == 0:
                @pl.when(core == 1)
                def _():
                    act(back_copy(dest, tau))
            else:
                act(back_copy(dest, tau))

    for copy in small:
        copy.wait()
    for h in range(2):
        for to in others(h):
            meta(h, to, mine[h]).start()
        trecv[h * 4 + mine[h]] = tv[h * 4 + mine[h]]
    scan[span] = jnp.zeros((half, low, width), jnp.float32)
    for i in range(2 * LOADS):
        load(i).wait()

    def compute(c):
        slot = c % PBUFS

        def one(i, last):
            p = steps[c, i]
            left = [occ[occ_idx[j, p]] for j in range(terms)]
            right = [virt[virt_idx[j, p]] for j in range(terms)]
            acc = jnp.dot(
                jnp.concatenate(left, axis=1),
                jnp.concatenate(right, axis=0),
                preferred_element_type=jnp.float32,
            )
            acc = acc + jnp.where(steps[c, per + i] != 0, last, 0.0)
            for g in range(groups):
                early[slot, g, i] = acc[g * rows:g * rows + low]
                upper = acc[g * rows + low:(g + 1) * rows]
                if g % 2 == 0:
                    timed[i, g // 2] = upper
                else:
                    late[c, g // 2, i] = upper
            return acc

        size = per // PARTS

        def portion(k, last):
            last = lax.fori_loop(
                0, size, lambda i, last: one(k * size + i, last), last,
                unroll=math.gcd(size, 4))
            for to in times():
                early_copy(c, to, tau, pl.ds(k * size, size)).start()
            return last

        lax.fori_loop(0, PARTS, portion, jnp.zeros((rows * groups, width), jnp.float32))

    def transform(landed, at):
        @pl.loop(0, per, unroll=2)
        def _(i):
            values = [landed[at, s, i] for s in range(groups)]
            for k in range(freqs):
                total = weights[k, 0] * values[0]
                for s in range(1, groups):
                    total += weights[k, s] * values[s]
                freq[i, k] = total

    def send_y(q, n, c, values):
        @pl.when(n >= outs[q])
        def _():
            for h in range(2):
                for to in others(h):
                    y_copy(q, n - outs[q], h, to, mine[h]).wait_send()

        @pl.loop(0, nz)
        def _(dz):
            for dy in range(ny):
                for m in range(each):
                    i = steps[c, 2 * per + (dz * ny + dy) * each + m]
                    leaving[q][n % outs[q], 0, dy, dz * each + m] = values[i, 0:half]
                    leaving[q][n % outs[q], 1, dz, dy * each + m] = values[i, half:freqs]

        for h in range(2):
            for to in others(h):
                y_copy(q, n, h, to, mine[h]).start()
            for e in range(slots):
                landing[q][n % ring[q], h, mine[h], e] = leaving[q][n % outs[q], h, mine[h], e]

    def tables():
        for h in range(2):
            for s in others(h):
                meta(h, s, s).wait_recv()
            for g in range(CHUNKS // GROUP):
                lane = lax.broadcasted_iota(jnp.int32, (share, width), 1)
                local = lax.broadcasted_iota(jnp.int32, (share, width), 0)
                goal = jnp.concatenate([
                    jnp.sum(jnp.where(lane == local + g * share, trecv[h * 4 + s][0:1], 0),
                            axis=1, keepdims=True) for s in range(sizes[h])], axis=0)
                index = lax.broadcasted_iota(jnp.int32, (span, 1), 0)
                valid = goal >= 0
                goal = jnp.where(valid, goal, 200)
                column = goal * 256 + index
                wide = (span, 2 * width)
                across = lax.broadcasted_iota(jnp.int32, wide, 1)
                down = lax.broadcasted_iota(jnp.int32, wide, 0)
                column_w = jnp.broadcast_to(column, wide)
                goal_w = jnp.broadcast_to(goal, wide)
                row = jnp.sum(jnp.where(across == down, column_w, 0), axis=0, keepdims=True)
                row_goal = jnp.sum(jnp.where(across == down, goal_w, 0), axis=0, keepdims=True)
                before = (row < column_w) & (across < span)
                rank = jnp.sum(jnp.where(before, 1, 0), axis=1, keepdims=True)
                joined = jnp.max(jnp.where(before & (row_goal == goal_w), 1, 0),
                                 axis=1, keepdims=True)
                entry = index + 1024 * joined
                entry = jnp.sum(jnp.where(rank == across, entry, 0), axis=0, keepdims=True)
                at = h * (CHUNKS // GROUP) + g
                order_v[at:at + 1] = entry
                found = jnp.where((goal == across[:, :width]) & valid, rank, -1)
                found = jnp.max(found, axis=0, keepdims=True)
                found = jnp.where(found < 0, span, found)
                spot_v[at:at + 1] = found
        for i, (source, into) in enumerate(((order_v, order), (spot_v, spot))):
            copy = pltpu.make_async_copy(source, into, tbl_sem.at[i])
            copy.start()
            copy.wait()

    def collect(q, n):
        for h in range(2):
            for s in others(h):
                y_copy(q, n, h, s, s).wait_recv()
            for s in range(sizes[h]):
                for e in range(slots):
                    work[q, h, s * share + e * GROUP + n % GROUP] = landing[q][n % ring[q], h, s, e]

    def densify(q, stream, g):
        for h in range(2):
            at = h * (CHUNKS // GROUP) + g

            def one(r, last):
                entry = order[at, r]
                value = work[q, h, entry & 1023]
                value = value + jnp.where(entry >= 1024, last, 0.0)
                scan[r] = value
                return value

            lax.fori_loop(0, span, one, jnp.zeros((half, low, width), jnp.float32), unroll=8)

            @pl.loop(0, sizes[1 - h])
            def _(o):
                @pl.loop(0, CHI_DEV, unroll=8)
                def _(e):
                    value = scan[spot[at, o * CHI_DEV + e]]
                    if g:
                        value = value + dense[stream, h, o, e]
                    dense[stream, h, o, e] = value

    def send_z(q):
        for h in range(2):
            for to in others(1 - h):
                z_copy(q, h, to, mine[1 - h]).start()

    def finish(q, store):
        for h in range(2):
            for s in others(1 - h):
                z_copy(q, h, s, s).wait_recv()
            own = mine[1 - h]

            @pl.loop(0, CHI_DEV, unroll=4)
            def _(e):
                total = dense[q, h, own, e]
                for s in others(1 - h):
                    total += zrecv[q, h, s, e]
                for k in range(half):
                    store(h * half + k, e, total[k])

    def store_early(k, e, value):
        out[k, e, 0:low] = value

    def store_late(k, e, value):
        out[k, e, low:rows] = value

    def store_final(k, e, value):
        final[k, e] = value

    def when(condition):
        return pl.when(condition)

    @pl.loop(0, 2 * rounds + 2 + LATER)
    def _(t):
        @when(t < rounds)
        def _():
            @when(t >= PBUFS)
            def _():
                for to in times():
                    early_copy(t - PBUFS, to, tau).wait_send()
            compute(t)

        @when(t == rounds - 1)
        def _():
            @pl.loop(0, rounds)
            def _(c):
                late_each(c, lambda copy: copy.start())

        @when(t < rounds)
        def _():
            send_y(1, t, t, timed)

            @pl.loop(0, per, unroll=4)
            def _(i):
                x_early[t % XRING, tau, i] = early[t % PBUFS, tau, i]

        @when((t >= 2) & (t < rounds + 2))
        def _():
            c = t - 2
            for s in times():
                early_copy(c, s, s).wait_recv()
            transform(x_early, c % XRING)
            send_y(0, c, c, freq)

        @when((t >= rounds + 2) & (t < 2 * rounds + 2) & (core == 1))
        def _():
            c = t - rounds - 2

            @pl.loop(0, per, unroll=4)
            def _(i):
                x_late[c, tau, i] = late[c, x, i]
            for s in times():
                late_copy(c, x, s).wait_recv()
            transform(x_late, c)
            send_y(1, c + rounds, c, freq)

        @when(t == 3)
        def _():
            tables()

        @when((t >= 2) & (t < rounds + 2))
        def _():
            collect(1, t - 2)

        @when(t == GROUP + 1)
        def _():
            densify(1, 2, 0)

        @when(t == rounds + 1)
        def _():
            densify(1, 2, 1)

        @when((t >= 4) & (t < rounds + 2))
        def _():
            collect(0, t - 4)

        @when(t == GROUP + 3)
        def _():
            densify(0, 0, 0)

        @when(t == rounds + 1)
        def _():
            send_z(2)

        @when(t == rounds + 3)
        def _():
            collect(0, rounds - 2)
            collect(0, rounds - 1)
            densify(0, 0, 1)

        @when(t == jnp.where(core == 1, rounds + ZLATE, rounds + 3))
        def _():
            send_z(0)

        @when(t == rounds + FSTEP)
        def _():
            finish(2, store_final)
            back_each(lambda copy: copy.start())

        @when((t >= rounds + 2 + LATER) & (core == 1))
        def _():
            collect(1, t - 2 - LATER)

        @when((t == rounds + 1 + LATER + GROUP) & (core == 1))
        def _():
            densify(1, 1, 0)

    @when(core == 1)
    def _():
        densify(1, 1, 1)
        send_z(1)

    finish(0, store_early)

    @when(core == 1)
    def _():
        finish(1, store_late)

    @when(core == 0)
    def _():
        @pl.loop(0, CHI_DEV, unroll=4)
        def _(e):
            back[tau, e] = final[x, e]
        for s in times():
            back_copy(x, s).wait_recv()

        @pl.loop(0, CHI_DEV, unroll=2)
        def _(e):
            values = [back[s, e] for s in range(groups)]
            for k in range(freqs):
                total = weights[k, 0] * values[0]
                for s in range(1, groups):
                    total += weights[k, s] * values[s]
                out[k, e, low:rows] = total

    def drain_z(q):
        for h in range(2):
            for to in others(1 - h):
                z_copy(q, h, to, mine[1 - h]).wait_send()

    def drain_y(q):
        for h in range(2):
            for n in range(outs[q]):
                for to in others(h):
                    y_copy(q, n, h, to, mine[h]).wait_send()

    for h in range(2):
        for to in others(h):
            meta(h, to, mine[h]).wait_send()
    drain_z(2)
    drain_z(0)
    drain_y(0)
    drain_y(1)
    pl.when(core == 1)(lambda: drain_z(1))
    back_each(lambda copy: copy.wait_send())

    @pl.loop(0, rounds)
    def _(c):
        late_each(c, lambda copy: copy.wait_send())

    @pl.loop(rounds - PBUFS, rounds)
    def _(c):
        for to in times():
            early_copy(c, to, tau).wait_send()


def plan(target, owners, ny, nz):
    count = target.shape[0]
    per = count // CHUNKS
    each = CAP // CHUNKS
    index = jnp.arange(count, dtype=jnp.int32)
    key = target * 256 + index
    rank = jnp.sum((key[None, :] < key[:, None]).astype(jnp.int32), axis=1)
    at = jnp.arange(per)[None, :] * CHUNKS + jnp.arange(CHUNKS)[:, None]
    ordered = jnp.sum(jnp.where(rank == at[..., None], key, 0), axis=2)
    part = ordered & 255
    tile = ordered >> 8
    same = (tile[:, 1:] == tile[:, :-1]).astype(jnp.int32)
    none = jnp.zeros((CHUNKS, 1), jnp.int32)
    keep = jnp.concatenate([none, same], axis=1)
    last = 1 - jnp.concatenate([same, none], axis=1)
    owner = tile // CHI_DEV
    value = jnp.where(last != 0, tile - owner * CHI_DEV, -1)
    j = jnp.arange(owners * each, dtype=jnp.int32)
    d, m = j // each, j % each
    place = jnp.sum((owner[:, None, :] < d[None, :, None]).astype(jnp.int32), axis=2) + m
    within = jnp.arange(per, dtype=jnp.int32)
    hit = (place[..., None] == within) & (owner[:, None, :] == d[None, :, None])
    goal = jnp.sum(jnp.where(hit, value[:, None, :] + 1, 0), axis=2) - 1
    place = jnp.minimum(place, per - 1)
    goal = goal.reshape(CHUNKS // GROUP, GROUP, nz, ny, each)
    zs = jnp.arange(nz, dtype=jnp.int32)[:, None, None] * CHI_DEV
    ys = jnp.arange(ny, dtype=jnp.int32)[None, :, None] * CHI_DEV
    to_y = jnp.where(goal >= 0, goal + zs, -1).transpose(3, 0, 2, 4, 1).reshape(ny, -1)
    to_z = jnp.where(goal >= 0, goal + ys, -1).transpose(2, 0, 3, 4, 1).reshape(nz, -1)
    both = jnp.concatenate([to_y, to_z])
    both = jnp.pad(both, ((0, 0), (0, 128 - both.shape[1])))
    both = jnp.broadcast_to(both[:, None], (both.shape[0], 8, 128))
    return jnp.concatenate([part, keep, place], axis=1), both


def body(occupied, virtual, cos_weights, pair_occ, pair_virt, partial_target_tile):
    owners = lax.axis_size("tile")
    groups = lax.axis_size("tau")
    size = occupied.shape[2]
    terms = pair_occ.shape[1]
    count = partial_target_tile.shape[0]
    freqs = cos_weights.shape[0]
    ny = 1
    while 2 * ny * 2 * ny <= owners:
        ny *= 2
    nz = owners // ny
    rows = size // groups
    per = count // CHUNKS
    slots = ny * (CAP // CHUNKS)
    half = freqs // 2
    low = rows // 2
    nx = groups // 2
    span = ny * slots * GROUP
    steps, both = plan(partial_target_tile, owners, ny, nz)
    vmem = pl.BlockSpec(memory_space=pltpu.VMEM)
    dma = pltpu.SemaphoreType.DMA
    f32 = jnp.float32
    return pl.pallas_call(
        functools.partial(main_kernel, ny, nz, groups, terms),
        out_shape=jax.ShapeDtypeStruct((freqs, CHI_DEV, rows, size), f32),
        in_specs=[pl.BlockSpec(memory_space=pl.ANY)] * 7,
        out_specs=vmem,
        scratch_shapes=[
            pltpu.VMEM(occupied.shape[1:], occupied.dtype),
            pltpu.VMEM(virtual.shape[1:], virtual.dtype),
            pltpu.SMEM(cos_weights.shape, f32),
            pltpu.SMEM((terms, count), jnp.int32),
            pltpu.SMEM((terms, count), jnp.int32),
            pltpu.SMEM(steps.shape, jnp.int32),
            pltpu.VMEM(both.shape, jnp.int32),
            pltpu.VMEM((PBUFS, groups, per, low, size), f32),
            pltpu.VMEM((CHUNKS, nx, per, low, size), f32),
            pltpu.VMEM((per, nx, low, size), f32),
            pltpu.VMEM((XRING, groups, per, low, size), f32),
            pltpu.VMEM((CHUNKS, groups, per, low, size), f32),
            pltpu.VMEM((per, freqs, low, size), f32),
            pltpu.VMEM((YBUFS[0], 2, ny, slots, half, low, size), f32),
            pltpu.VMEM((YBUFS[1], 2, ny, slots, half, low, size), f32),
            pltpu.VMEM((RINGS[0], 2, ny, slots, half, low, size), f32),
            pltpu.VMEM((RINGS[1], 2, ny, slots, half, low, size), f32),
            pltpu.VMEM((2, 2, span, half, low, size), f32),
            pltpu.VMEM((span + 1, half, low, size), f32),
            pltpu.VMEM((3, 2, ny, CHI_DEV, half, low, size), f32),
            pltpu.VMEM((3, 2, ny, CHI_DEV, half, low, size), f32),
            pltpu.VMEM((nx, CHI_DEV, low, size), f32),
            pltpu.VMEM((groups, CHI_DEV, low, size), f32),
            pltpu.VMEM((8, 8, size), jnp.int32),
            pltpu.VMEM((8, 2 * size), jnp.int32),
            pltpu.VMEM((8, size), jnp.int32),
            pltpu.SMEM((8, 2 * size), jnp.int32),
            pltpu.SMEM((8, size), jnp.int32),
            dma((PBUFS * groups,)),
            dma((XRING * groups,)),
            dma((CHUNKS * nx,)),
            dma((CHUNKS * groups,)),
            dma((sum(YBUFS) * 8,)),
            dma((sum(RINGS) * 8,)),
            dma((3 * 8,)),
            dma((3 * 8,)),
            dma((nx,)),
            dma((groups,)),
            dma((8,)),
            dma((8,)),
            dma((2,)),
            dma((2 * LOADS + 5,)),
        ],
        compiler_params=pltpu.CompilerParams(
            collective_id=0, has_side_effects=True, vmem_limit_bytes=67043328),
    )(cos_weights, pair_occ.T, pair_virt.T, steps,
      both, occupied[0], virtual[0])


def solution(mesh):
    in_specs = (
        P("tau", "tile", None, None),
        P("tau", "tile", None, None),
        P(),
        P("tile", None),
        P("tile", None),
        P("tile"),
    )
    out_specs = P(None, "tile", "tau", None)
    return jax.shard_map(body, mesh=mesh, in_specs=in_specs, out_specs=out_specs, check_vma=False)
```

```python
import functools
import math

import jax
import jax.numpy as jnp
from jax import lax
from jax.experimental import pallas as pl
from jax.experimental.pallas import tpu as pltpu
from jax.sharding import PartitionSpec as P

CHI_DEV = 32
CAP = 24
CHUNKS = 8
PBUFS = 4
YBUFS = (2, 4)
RINGS = (6, 8)
XRING = 6
PARTS = 6
GROUP = 4
LATER = 7
FSTEP = 7
ZSOON = 5
ZLATE = 9
LOADS = 4
MESH = pl.DeviceIdType.MESH


def main_kernel(ny, nz, groups, terms,
                weights_in, occ_idx_in, virt_idx_in, tables_in, occ_hbm, virt_hbm,
                out,
                occ, virt, weights, occ_idx, virt_idx, steps, tv, early, late, timed, x_early, x_late, freq, y_out_first, y_out_second, y_first, y_second, work, scan, dense, zrecv,
                final, back, trecv, order_v, spot_v, order, spot,
                e_send, e_recv, l_send, l_recv, y_send, y_recv, z_send, z_recv,
                b_send, b_recv, t_send, t_recv, tbl_sem, load_sem):
    tau = lax.axis_index("tau")
    tile = lax.axis_index("tile")
    x, core = tau // 2, tau % 2
    nx = groups // 2
    z, y = tile // ny, tile % ny
    mine = (y, z)
    sizes = (ny, nz)
    freqs, _, rows, width = out.shape
    low = rows // 2
    half = freqs // 2
    per = freq.shape[0]
    slots = y_first.shape[3]
    each = slots // ny
    rounds = CHUNKS
    span = work.shape[2]
    share = slots * GROUP

    def peer(h, i):
        return {"tile": z * ny + i if h == 0 else i * ny + y}

    def others(h):
        return [(mine[h] + step) % sizes[h] for step in range(1, sizes[h])]

    def times():
        return [(tau + step) % groups for step in range(1, groups)]

    landing = (y_first, y_second)
    ring = (y_first.shape[0], y_second.shape[0])
    base = (0, ring[0])
    leaving = (y_out_first, y_out_second)
    outs = (y_out_first.shape[0], y_out_second.shape[0])
    out_base = (0, outs[0])
    part_size = occ.shape[0] // LOADS

    def load(i):
        at = pl.ds(i % LOADS * part_size, part_size)
        source, into = ((occ_hbm, occ), (virt_hbm, virt))[i // LOADS]
        return pltpu.make_async_copy(source.at[at], into.at[at], load_sem.at[i])

    small = [
        pltpu.make_async_copy(source, into, load_sem.at[2 * LOADS + i])
        for i, (source, into) in enumerate((
            (tables_in.at[pl.ds(0, 8)], tv), (occ_idx_in, occ_idx), (virt_idx_in, virt_idx),
            (tables_in.at[8], steps), (weights_in, weights)))
    ]
    for copy in small:
        copy.start()
    for i in range(2 * LOADS):
        load(i).start()

    barrier = pltpu.get_barrier_semaphore()
    for to in times():
        pl.semaphore_signal(barrier, inc=1, device_id={"tau": to}, device_id_type=MESH)
    for h in range(2):
        for to in others(h):
            pl.semaphore_signal(barrier, inc=1, device_id=peer(h, to), device_id_type=MESH)
    pl.semaphore_wait(barrier, groups - 1 + ny - 1 + nz - 1)

    def meta(h, to, at):
        return pltpu.make_async_remote_copy(
            src_ref=tv.at[h * 4 + to], dst_ref=trecv.at[h * 4 + mine[h]],
            send_sem=t_send.at[h * 4 + to], recv_sem=t_recv.at[h * 4 + at],
            device_id=peer(h, to), device_id_type=MESH)

    def early_copy(c, to, source, at=None):
        at = pl.ds(0, per) if at is None else at
        return pltpu.make_async_remote_copy(
            src_ref=early.at[c % PBUFS, to, at], dst_ref=x_early.at[c % XRING, source, at],
            send_sem=e_send.at[c % PBUFS * groups + to],
            recv_sem=e_recv.at[c % XRING * groups + source],
            device_id={"tau": to}, device_id_type=MESH)

    def late_copy(c, dest, source):
        return pltpu.make_async_remote_copy(
            src_ref=late.at[c, dest], dst_ref=x_late.at[c, source],
            send_sem=l_send.at[c * nx + dest],
            recv_sem=l_recv.at[c * groups + source],
            device_id={"tau": 2 * dest + 1}, device_id_type=MESH)

    def late_each(c, act):
        for step in range(nx):
            dest = (x + step) % nx
            if step == 0:
                @pl.when(core == 0)
                def _():
                    act(late_copy(c, dest, tau))
            else:
                act(late_copy(c, dest, tau))

    def y_copy(q, n, h, to, source):
        return pltpu.make_async_remote_copy(
            src_ref=leaving[q].at[n % outs[q], h, to], dst_ref=landing[q].at[n % ring[q], h, source],
            send_sem=y_send.at[((out_base[q] + n % outs[q]) * 2 + h) * 4 + to],
            recv_sem=y_recv.at[((base[q] + n % ring[q]) * 2 + h) * 4 + source],
            device_id=peer(h, to), device_id_type=MESH)

    def z_copy(q, h, to, source):
        return pltpu.make_async_remote_copy(
            src_ref=dense.at[q, h, to], dst_ref=zrecv.at[q, h, source],
            send_sem=z_send.at[(q * 2 + h) * 4 + to],
            recv_sem=z_recv.at[(q * 2 + h) * 4 + source],
            device_id=peer(1 - h, to), device_id_type=MESH)

    def around(h):
        i, n = mine[1 - h], sizes[1 - h]
        return i, (i + 1) % n, (i + 2) % n, (i + 3) % n

    def relay_copy(q, h, right, landed):
        i, after, across, before = around(h)
        into = i if landed else (after if right else before)
        mid = CHI_DEV // 2
        at = pl.ds(0 if right else mid, mid)
        row = (q * 2 + h) * 4
        return pltpu.make_async_remote_copy(
            src_ref=dense.at[q, h, across, at], dst_ref=zrecv.at[q, h, into, at],
            send_sem=z_send.at[row + (across if right else i)],
            recv_sem=z_recv.at[row + (into if right else (into + 2) % sizes[1 - h])],
            device_id=peer(1 - h, after if right else before), device_id_type=MESH)

    def back_copy(dest, source):
        return pltpu.make_async_remote_copy(
            src_ref=final.at[dest], dst_ref=back.at[source],
            send_sem=b_send.at[dest], recv_sem=b_recv.at[source],
            device_id={"tau": 2 * dest}, device_id_type=MESH)

    def back_each(act):
        for step in range(nx):
            dest = (x + step) % nx
            if step == 0:
                @pl.when(core == 1)
                def _():
                    act(back_copy(dest, tau))
            else:
                act(back_copy(dest, tau))

    for copy in small:
        copy.wait()
    for h in range(2):
        for to in others(h):
            meta(h, to, mine[h]).start()
        trecv[h * 4 + mine[h]] = tv[h * 4 + mine[h]]
    scan[span] = jnp.zeros((half, low, width), jnp.float32)
    for i in range(2 * LOADS):
        load(i).wait()

    def compute(c):
        slot = c % PBUFS

        def one(i, last):
            p = steps[c, i]
            left = [occ[occ_idx[j, p]] for j in range(terms)]
            right = [virt[virt_idx[j, p]] for j in range(terms)]
            acc = jnp.dot(
                jnp.concatenate(left, axis=1),
                jnp.concatenate(right, axis=0),
                preferred_element_type=jnp.float32,
            )
            acc = acc + jnp.where(steps[c, per + i] != 0, last, 0.0)
            for g in range(groups):
                early[slot, g, i] = acc[g * rows:g * rows + low]
                upper = acc[g * rows + low:(g + 1) * rows]
                if g % 2 == 0:
                    timed[i, g // 2] = upper
                else:
                    late[c, g // 2, i] = upper
            return acc

        size = per // PARTS

        def portion(k, last):
            last = lax.fori_loop(
                0, size, lambda i, last: one(k * size + i, last), last,
                unroll=math.gcd(size, 4))
            for to in times():
                early_copy(c, to, tau, pl.ds(k * size, size)).start()
            return last

        lax.fori_loop(0, PARTS, portion, jnp.zeros((rows * groups, width), jnp.float32))

    def transform(landed, at):
        @pl.loop(0, per, unroll=2)
        def _(i):
            values = [landed[at, s, i] for s in range(groups)]
            for k in range(freqs):
                total = weights[k, 0] * values[0]
                for s in range(1, groups):
                    total += weights[k, s] * values[s]
                freq[i, k] = total

    def send_y(q, n, c, values):
        @pl.when(n >= outs[q])
        def _():
            for h in range(2):
                for to in others(h):
                    y_copy(q, n - outs[q], h, to, mine[h]).wait_send()

        @pl.loop(0, nz)
        def _(dz):
            for dy in range(ny):
                for m in range(each):
                    i = steps[c, 2 * per + (dz * ny + dy) * each + m]
                    leaving[q][n % outs[q], 0, dy, dz * each + m] = values[i, 0:half]
                    leaving[q][n % outs[q], 1, dz, dy * each + m] = values[i, half:freqs]

        for h in range(2):
            for to in others(h):
                y_copy(q, n, h, to, mine[h]).start()
            for e in range(slots):
                landing[q][n % ring[q], h, mine[h], e] = leaving[q][n % outs[q], h, mine[h], e]

    def tables():
        for h in range(2):
            for s in others(h):
                meta(h, s, s).wait_recv()
            for g in range(CHUNKS // GROUP):
                lane = lax.broadcasted_iota(jnp.int32, (share, width), 1)
                local = lax.broadcasted_iota(jnp.int32, (share, width), 0)
                goal = jnp.concatenate([
                    jnp.sum(jnp.where(lane == local + g * share, trecv[h * 4 + s][0:1], 0),
                            axis=1, keepdims=True) for s in range(sizes[h])], axis=0)
                index = lax.broadcasted_iota(jnp.int32, (span, 1), 0)
                valid = goal >= 0
                goal = jnp.where(valid, goal, 200)
                column = goal * 256 + index
                wide = (span, 2 * width)
                across = lax.broadcasted_iota(jnp.int32, wide, 1)
                down = lax.broadcasted_iota(jnp.int32, wide, 0)
                column_w = jnp.broadcast_to(column, wide)
                goal_w = jnp.broadcast_to(goal, wide)
                row = jnp.sum(jnp.where(across == down, column_w, 0), axis=0, keepdims=True)
                row_goal = jnp.sum(jnp.where(across == down, goal_w, 0), axis=0, keepdims=True)
                before = (row < column_w) & (across < span)
                rank = jnp.sum(jnp.where(before, 1, 0), axis=1, keepdims=True)
                joined = jnp.max(jnp.where(before & (row_goal == goal_w), 1, 0),
                                 axis=1, keepdims=True)
                entry = index + 1024 * joined
                entry = jnp.sum(jnp.where(rank == across, entry, 0), axis=0, keepdims=True)
                at = h * (CHUNKS // GROUP) + g
                order_v[at:at + 1] = entry
                found = jnp.where((goal == across[:, :width]) & valid, rank, -1)
                found = jnp.max(found, axis=0, keepdims=True)
                found = jnp.where(found < 0, span, found)
                spot_v[at:at + 1] = found
        for i, (source, into) in enumerate(((order_v, order), (spot_v, spot))):
            copy = pltpu.make_async_copy(source, into, tbl_sem.at[i])
            copy.start()
            copy.wait()

    def collect(q, n):
        for h in range(2):
            for s in others(h):
                y_copy(q, n, h, s, s).wait_recv()
            for s in range(sizes[h]):
                for e in range(slots):
                    work[q, h, s * share + e * GROUP + n % GROUP] = landing[q][n % ring[q], h, s, e]

    def densify(q, stream, g):
        for h in range(2):
            at = h * (CHUNKS // GROUP) + g

            def one(r, last):
                entry = order[at, r]
                value = work[q, h, entry & 1023]
                value = value + jnp.where(entry >= 1024, last, 0.0)
                scan[r] = value
                return value

            lax.fori_loop(0, span, one, jnp.zeros((half, low, width), jnp.float32), unroll=8)

            @pl.loop(0, sizes[1 - h])
            def _(o):
                @pl.loop(0, CHI_DEV, unroll=8)
                def _(e):
                    value = scan[spot[at, o * CHI_DEV + e]]
                    if g:
                        value = value + dense[stream, h, o, e]
                    dense[stream, h, o, e] = value

    def send_z(q):
        for h in range(2):
            for to in others(1 - h):
                z_copy(q, h, to, mine[1 - h]).start()

    def send_relay(q):
        for h in range(2):
            for right in (True, False):
                relay_copy(q, h, right, False).start()

    def send_merged(q):
        for h in range(2):
            i, after, across, before = around(h)
            mid = CHI_DEV // 2
            for right in (True, False):
                relay_copy(q, h, right, True).wait_recv()

            @pl.loop(0, mid, unroll=4)
            def _(e):
                dense[q, h, after, e] += zrecv[q, h, i, e]
                dense[q, h, before, mid + e] += zrecv[q, h, i, mid + e]
            z_copy(q, h, after, i).start()
            z_copy(q, h, before, i).start()

    def givers(q, h):
        i, after, across, before = around(h)
        return others(1 - h) if q == 1 else [after, before]

    def finish(q, store):
        for h in range(2):
            for s in givers(q, h):
                z_copy(q, h, s, s).wait_recv()
            own = mine[1 - h]

            @pl.loop(0, CHI_DEV, unroll=4)
            def _(e):
                total = dense[q, h, own, e]
                for s in givers(q, h):
                    total += zrecv[q, h, s, e]
                for k in range(half):
                    store(h * half + k, e, total[k])

    def store_early(k, e, value):
        out[k, e, 0:low] = value

    def store_late(k, e, value):
        out[k, e, low:rows] = value

    def store_final(k, e, value):
        final[k, e] = value

    def when(condition):
        return pl.when(condition)

    @pl.loop(0, 2 * rounds + 2 + LATER)
    def _(t):
        @when(t < rounds)
        def _():
            @when(t >= PBUFS)
            def _():
                for to in times():
                    early_copy(t - PBUFS, to, tau).wait_send()
            compute(t)

        @when(t == rounds - 1)
        def _():
            @pl.loop(0, rounds)
            def _(c):
                late_each(c, lambda copy: copy.start())

        @when(t < rounds)
        def _():
            send_y(1, t, t, timed)

            @pl.loop(0, per, unroll=4)
            def _(i):
                x_early[t % XRING, tau, i] = early[t % PBUFS, tau, i]

        @when((t >= 2) & (t < rounds + 2))
        def _():
            c = t - 2
            for s in times():
                early_copy(c, s, s).wait_recv()
            transform(x_early, c % XRING)
            send_y(0, c, c, freq)

        @when((t >= rounds + 2) & (t < 2 * rounds + 2) & (core == 1))
        def _():
            c = t - rounds - 2

            @pl.loop(0, per, unroll=4)
            def _(i):
                x_late[c, tau, i] = late[c, x, i]
            for s in times():
                late_copy(c, x, s).wait_recv()
            transform(x_late, c)
            send_y(1, c + rounds, c, freq)

        @when(t == 3)
        def _():
            tables()

        @when((t >= 2) & (t < rounds + 2))
        def _():
            collect(1, t - 2)

        @when(t == GROUP + 1)
        def _():
            densify(1, 2, 0)

        @when(t == rounds + 1)
        def _():
            densify(1, 2, 1)

        @when((t >= 4) & (t < rounds + 2))
        def _():
            collect(0, t - 4)

        @when(t == GROUP + 3)
        def _():
            densify(0, 0, 0)

        @when(t == rounds + 1)
        def _():
            send_relay(2)

        @when(t == rounds + 3)
        def _():
            collect(0, rounds - 2)
            collect(0, rounds - 1)
            densify(0, 0, 1)
            send_relay(0)
            send_merged(2)

        @when(t == jnp.where(core == 1, rounds + ZLATE, rounds + ZSOON))
        def _():
            send_merged(0)

        @when(t == rounds + FSTEP)
        def _():
            finish(2, store_final)
            back_each(lambda copy: copy.start())

        @when((t >= rounds + 2 + LATER) & (core == 1))
        def _():
            collect(1, t - 2 - LATER)

        @when((t == rounds + 1 + LATER + GROUP) & (core == 1))
        def _():
            densify(1, 1, 0)

    @when(core == 1)
    def _():
        densify(1, 1, 1)
        send_z(1)

    finish(0, store_early)

    @when(core == 1)
    def _():
        finish(1, store_late)

    @when(core == 0)
    def _():
        @pl.loop(0, CHI_DEV, unroll=4)
        def _(e):
            back[tau, e] = final[x, e]
        for s in times():
            back_copy(x, s).wait_recv()

        @pl.loop(0, CHI_DEV, unroll=2)
        def _(e):
            values = [back[s, e] for s in range(groups)]
            for k in range(freqs):
                total = weights[k, 0] * values[0]
                for s in range(1, groups):
                    total += weights[k, s] * values[s]
                out[k, e, low:rows] = total

    def drain_z(q):
        for h in range(2):
            for to in givers(q, h):
                z_copy(q, h, to, mine[1 - h]).wait_send()
            if q != 1:
                for right in (True, False):
                    relay_copy(q, h, right, False).wait_send()

    def drain_y(q):
        for h in range(2):
            for n in range(outs[q]):
                for to in others(h):
                    y_copy(q, n, h, to, mine[h]).wait_send()

    for h in range(2):
        for to in others(h):
            meta(h, to, mine[h]).wait_send()
    drain_z(2)
    drain_z(0)
    drain_y(0)
    drain_y(1)
    pl.when(core == 1)(lambda: drain_z(1))
    back_each(lambda copy: copy.wait_send())

    @pl.loop(0, rounds)
    def _(c):
        late_each(c, lambda copy: copy.wait_send())

    @pl.loop(rounds - PBUFS, rounds)
    def _(c):
        for to in times():
            early_copy(c, to, tau).wait_send()


def plan(target, owners, ny, nz):
    count = target.shape[0]
    per = count // CHUNKS
    each = CAP // CHUNKS
    index = jnp.arange(count, dtype=jnp.int32)
    key = target * 256 + index
    rank = jnp.sum((key[None, :] < key[:, None]).astype(jnp.int32), axis=1)
    at = jnp.arange(per)[None, :] * CHUNKS + jnp.arange(CHUNKS)[:, None]
    ordered = jnp.sum(jnp.where(rank == at[..., None], key, 0), axis=2)
    part = ordered & 255
    tile = ordered >> 8
    same = (tile[:, 1:] == tile[:, :-1]).astype(jnp.int32)
    none = jnp.zeros((CHUNKS, 1), jnp.int32)
    keep = jnp.concatenate([none, same], axis=1)
    last = 1 - jnp.concatenate([same, none], axis=1)
    owner = tile // CHI_DEV
    value = jnp.where(last != 0, tile - owner * CHI_DEV, -1)
    j = jnp.arange(owners * each, dtype=jnp.int32)
    d, m = j // each, j % each
    place = jnp.sum((owner[:, None, :] < d[None, :, None]).astype(jnp.int32), axis=2) + m
    within = jnp.arange(per, dtype=jnp.int32)
    hit = (place[..., None] == within) & (owner[:, None, :] == d[None, :, None])
    goal = jnp.sum(jnp.where(hit, value[:, None, :] + 1, 0), axis=2) - 1
    place = jnp.minimum(place, per - 1)
    goal = goal.reshape(CHUNKS // GROUP, GROUP, nz, ny, each)
    zs = jnp.arange(nz, dtype=jnp.int32)[:, None, None] * CHI_DEV
    ys = jnp.arange(ny, dtype=jnp.int32)[None, :, None] * CHI_DEV
    to_y = jnp.where(goal >= 0, goal + zs, -1).transpose(3, 0, 2, 4, 1).reshape(ny, -1)
    to_z = jnp.where(goal >= 0, goal + ys, -1).transpose(2, 0, 3, 4, 1).reshape(nz, -1)
    both = jnp.concatenate([to_y, to_z])
    both = jnp.pad(both, ((0, 0), (0, 128 - both.shape[1])))
    both = jnp.broadcast_to(both[:, None], (both.shape[0], 8, 128))
    steps = jnp.concatenate([part, keep, place], axis=1)
    steps = jnp.pad(steps, ((0, 0), (0, 128 - steps.shape[1])))
    return jnp.concatenate([both, steps[None]])


def body(occupied, virtual, cos_weights, pair_occ, pair_virt, partial_target_tile):
    owners = lax.axis_size("tile")
    groups = lax.axis_size("tau")
    size = occupied.shape[2]
    terms = pair_occ.shape[1]
    count = partial_target_tile.shape[0]
    freqs = cos_weights.shape[0]
    ny = 1
    while 2 * ny * 2 * ny <= owners:
        ny *= 2
    nz = owners // ny
    rows = size // groups
    per = count // CHUNKS
    slots = ny * (CAP // CHUNKS)
    half = freqs // 2
    low = rows // 2
    nx = groups // 2
    span = ny * slots * GROUP
    both = plan(partial_target_tile, owners, ny, nz)
    vmem = pl.BlockSpec(memory_space=pltpu.VMEM)
    dma = pltpu.SemaphoreType.DMA
    f32 = jnp.float32
    return pl.pallas_call(
        functools.partial(main_kernel, ny, nz, groups, terms),
        out_shape=jax.ShapeDtypeStruct((freqs, CHI_DEV, rows, size), f32),
        in_specs=[pl.BlockSpec(memory_space=pl.ANY)] * 6,
        out_specs=vmem,
        scratch_shapes=[
            pltpu.VMEM(occupied.shape[1:], occupied.dtype),
            pltpu.VMEM(virtual.shape[1:], virtual.dtype),
            pltpu.SMEM(cos_weights.shape, f32),
            pltpu.SMEM((terms, count), jnp.int32),
            pltpu.SMEM((terms, count), jnp.int32),
            pltpu.SMEM(both.shape[1:], jnp.int32),
            pltpu.VMEM((8,) + both.shape[1:], jnp.int32),
            pltpu.VMEM((PBUFS, groups, per, low, size), f32),
            pltpu.VMEM((CHUNKS, nx, per, low, size), f32),
            pltpu.VMEM((per, nx, low, size), f32),
            pltpu.VMEM((XRING, groups, per, low, size), f32),
            pltpu.VMEM((CHUNKS, groups, per, low, size), f32),
            pltpu.VMEM((per, freqs, low, size), f32),
            pltpu.VMEM((YBUFS[0], 2, ny, slots, half, low, size), f32),
            pltpu.VMEM((YBUFS[1], 2, ny, slots, half, low, size), f32),
            pltpu.VMEM((RINGS[0], 2, ny, slots, half, low, size), f32),
            pltpu.VMEM((RINGS[1], 2, ny, slots, half, low, size), f32),
            pltpu.VMEM((2, 2, span, half, low, size), f32),
            pltpu.VMEM((span + 1, half, low, size), f32),
            pltpu.VMEM((3, 2, ny, CHI_DEV, half, low, size), f32),
            pltpu.VMEM((3, 2, ny, CHI_DEV, half, low, size), f32),
            pltpu.VMEM((nx, CHI_DEV, low, size), f32),
            pltpu.VMEM((groups, CHI_DEV, low, size), f32),
            pltpu.VMEM((8, 8, size), jnp.int32),
            pltpu.VMEM((8, 2 * size), jnp.int32),
            pltpu.VMEM((8, size), jnp.int32),
            pltpu.SMEM((8, 2 * size), jnp.int32),
            pltpu.SMEM((8, size), jnp.int32),
            dma((PBUFS * groups,)),
            dma((XRING * groups,)),
            dma((CHUNKS * nx,)),
            dma((CHUNKS * groups,)),
            dma((sum(YBUFS) * 8,)),
            dma((sum(RINGS) * 8,)),
            dma((3 * 8,)),
            dma((3 * 8,)),
            dma((nx,)),
            dma((groups,)),
            dma((8,)),
            dma((8,)),
            dma((2,)),
            dma((2 * LOADS + 5,)),
        ],
        compiler_params=pltpu.CompilerParams(
            collective_id=0, has_side_effects=True, vmem_limit_bytes=67043328),
    )(cos_weights, pair_occ.T, pair_virt.T, both,
      occupied[0], virtual[0])


def solution(mesh):
    in_specs = (
        P("tau", "tile", None, None),
        P("tau", "tile", None, None),
        P(),
        P("tile", None),
        P("tile", None),
        P("tile"),
    )
    out_specs = P(None, "tile", "tau", None)
    return jax.shard_map(body, mesh=mesh, in_specs=in_specs, out_specs=out_specs, check_vma=False)
```

```python
import functools
import math

import jax
import jax.numpy as jnp
from jax import lax
from jax.experimental import pallas as pl
from jax.experimental.pallas import tpu as pltpu
from jax.sharding import PartitionSpec as P

CHI_DEV = 32
CAP = 24
CHUNKS = 8
PBUFS = 4
YBUFS = (2, 4)
RINGS = (6, 8)
XRING = 6
PARTS = 6
GROUP = 4
LATER = 7
FSTEP = 7
ZSOON = 5
ZLATE = 9
LOADS = 4
MESH = pl.DeviceIdType.MESH


def main_kernel(ny, nz, groups, terms,
                weights_in, occ_idx_in, virt_idx_in, tables_in, occ_hbm, virt_hbm,
                out,
                occ, virt, weights, occ_idx, virt_idx, steps, tv, early, late, timed, x_early, x_late, freq, y_out_first, y_out_second, y_first, y_second, work, scan, dense, zrecv,
                final, back, trecv, order_v, spot_v, order, spot,
                e_send, e_recv, l_send, l_recv, y_send, y_recv, z_send, z_recv,
                b_send, b_recv, t_send, t_recv, tbl_sem, load_sem):
    tau = lax.axis_index("tau")
    tile = lax.axis_index("tile")
    x, core = tau // 2, tau % 2
    nx = groups // 2
    z, y = tile // ny, tile % ny
    mine = (y, z)
    sizes = (ny, nz)
    freqs, _, rows, width = out.shape
    low = rows // 2
    half = freqs // 2
    per = freq.shape[0]
    slots = y_first.shape[3]
    each = slots // ny
    rounds = CHUNKS
    span = work.shape[2]
    share = slots * GROUP

    def peer(h, i):
        return {"tile": z * ny + i if h == 0 else i * ny + y}

    def others(h):
        return [(mine[h] + step) % sizes[h] for step in range(1, sizes[h])]

    def times():
        return [(tau + step) % groups for step in range(1, groups)]

    landing = (y_first, y_second)
    ring = (y_first.shape[0], y_second.shape[0])
    base = (0, ring[0])
    leaving = (y_out_first, y_out_second)
    outs = (y_out_first.shape[0], y_out_second.shape[0])
    out_base = (0, outs[0])
    part_size = occ.shape[0] // LOADS

    def load(i):
        at = pl.ds(i % LOADS * part_size, part_size)
        source, into = ((occ_hbm, occ), (virt_hbm, virt))[i // LOADS]
        return pltpu.make_async_copy(source.at[at], into.at[at], load_sem.at[i])

    small = [
        pltpu.make_async_copy(source, into, load_sem.at[2 * LOADS + i])
        for i, (source, into) in enumerate((
            (tables_in.at[pl.ds(0, 8)], tv), (occ_idx_in, occ_idx), (virt_idx_in, virt_idx),
            (tables_in.at[8], steps), (weights_in, weights)))
    ]
    for copy in small:
        copy.start()
    for i in range(2 * LOADS):
        load(i).start()

    barrier = pltpu.get_barrier_semaphore()
    for to in times():
        pl.semaphore_signal(barrier, inc=1, device_id={"tau": to}, device_id_type=MESH)
    for h in range(2):
        for to in others(h):
            pl.semaphore_signal(barrier, inc=1, device_id=peer(h, to), device_id_type=MESH)
    pl.semaphore_wait(barrier, groups - 1 + ny - 1 + nz - 1)

    def meta(h, to, at):
        return pltpu.make_async_remote_copy(
            src_ref=tv.at[h * 4 + to], dst_ref=trecv.at[h * 4 + mine[h]],
            send_sem=t_send.at[h * 4 + to], recv_sem=t_recv.at[h * 4 + at],
            device_id=peer(h, to), device_id_type=MESH)

    def early_copy(c, to, source, at=None):
        at = pl.ds(0, per) if at is None else at
        return pltpu.make_async_remote_copy(
            src_ref=early.at[c % PBUFS, to, at], dst_ref=x_early.at[c % XRING, source, at],
            send_sem=e_send.at[c % PBUFS * groups + to],
            recv_sem=e_recv.at[c % XRING * groups + source],
            device_id={"tau": to}, device_id_type=MESH)

    def late_copy(c, dest, source):
        return pltpu.make_async_remote_copy(
            src_ref=late.at[c, dest], dst_ref=x_late.at[c, source],
            send_sem=l_send.at[c * nx + dest],
            recv_sem=l_recv.at[c * groups + source],
            device_id={"tau": 2 * dest + 1}, device_id_type=MESH)

    def late_each(c, act):
        for step in range(nx):
            dest = (x + step) % nx
            if step == 0:
                @pl.when(core == 0)
                def _():
                    act(late_copy(c, dest, tau))
            else:
                act(late_copy(c, dest, tau))

    def y_copy(q, n, h, to, source):
        return pltpu.make_async_remote_copy(
            src_ref=leaving[q].at[n % outs[q], h, to], dst_ref=landing[q].at[n % ring[q], h, source],
            send_sem=y_send.at[((out_base[q] + n % outs[q]) * 2 + h) * 4 + to],
            recv_sem=y_recv.at[((base[q] + n % ring[q]) * 2 + h) * 4 + source],
            device_id=peer(h, to), device_id_type=MESH)

    def z_copy(q, h, to, source):
        return pltpu.make_async_remote_copy(
            src_ref=dense.at[q, h, to], dst_ref=zrecv.at[q, h, source],
            send_sem=z_send.at[(q * 2 + h) * 4 + to],
            recv_sem=z_recv.at[(q * 2 + h) * 4 + source],
            device_id=peer(1 - h, to), device_id_type=MESH)

    def around(h):
        i, n = mine[1 - h], sizes[1 - h]
        return i, (i + 1) % n, (i + 2) % n, (i + 3) % n

    def relay_copy(q, h, right, landed):
        i, after, across, before = around(h)
        into = i if landed else (after if right else before)
        mid = CHI_DEV // 2
        at = pl.ds(0 if right else mid, mid)
        row = (q * 2 + h) * 4
        return pltpu.make_async_remote_copy(
            src_ref=dense.at[q, h, across, at], dst_ref=zrecv.at[q, h, into, at],
            send_sem=z_send.at[row + (across if right else i)],
            recv_sem=z_recv.at[row + (into if right else (into + 2) % sizes[1 - h])],
            device_id=peer(1 - h, after if right else before), device_id_type=MESH)

    def back_copy(dest, source):
        return pltpu.make_async_remote_copy(
            src_ref=final.at[dest], dst_ref=back.at[source],
            send_sem=b_send.at[dest], recv_sem=b_recv.at[source],
            device_id={"tau": 2 * dest}, device_id_type=MESH)

    def back_each(act):
        for step in range(nx):
            dest = (x + step) % nx
            if step == 0:
                @pl.when(core == 1)
                def _():
                    act(back_copy(dest, tau))
            else:
                act(back_copy(dest, tau))

    for copy in small:
        copy.wait()
    for h in range(2):
        for to in others(h):
            meta(h, to, mine[h]).start()
        trecv[h * 4 + mine[h]] = tv[h * 4 + mine[h]]
    scan[span] = jnp.zeros((half, low, width), jnp.float32)
    for i in range(2 * LOADS):
        load(i).wait()

    def compute(c):
        slot = c % PBUFS

        def one(i, last):
            p = steps[c, i]
            left = [occ[occ_idx[j, p]] for j in range(terms)]
            right = [virt[virt_idx[j, p]] for j in range(terms)]
            acc = jnp.dot(
                jnp.concatenate(left, axis=1),
                jnp.concatenate(right, axis=0),
                preferred_element_type=jnp.float32,
            )
            acc = acc + jnp.where(steps[c, per + i] != 0, last, 0.0)
            for g in range(groups):
                early[slot, g, i] = acc[g * rows:g * rows + low]
                upper = acc[g * rows + low:(g + 1) * rows]
                if g % 2 == 0:
                    timed[i, g // 2] = upper
                else:
                    late[c, g // 2, i] = upper
            return acc

        size = per // PARTS

        def portion(k, last):
            last = lax.fori_loop(
                0, size, lambda i, last: one(k * size + i, last), last,
                unroll=math.gcd(size, 4))
            for to in times():
                early_copy(c, to, tau, pl.ds(k * size, size)).start()
            return last

        lax.fori_loop(0, PARTS, portion, jnp.zeros((rows * groups, width), jnp.float32))

    def transform(landed, at):
        @pl.loop(0, per, unroll=2)
        def _(i):
            values = [landed[at, s, i] for s in range(groups)]
            for k in range(freqs):
                total = weights[k, 0] * values[0]
                for s in range(1, groups):
                    total += weights[k, s] * values[s]
                freq[i, k] = total

    def send_y(q, n, c, values):
        @pl.when(n >= outs[q])
        def _():
            for h in range(2):
                for to in others(h):
                    y_copy(q, n - outs[q], h, to, mine[h]).wait_send()

        @pl.loop(0, nz)
        def _(dz):
            for dy in range(ny):
                for m in range(each):
                    i = steps[c, 2 * per + (dz * ny + dy) * each + m]
                    leaving[q][n % outs[q], 0, dy, dz * each + m] = values[i, 0:half]
                    leaving[q][n % outs[q], 1, dz, dy * each + m] = values[i, half:freqs]

        for h in range(2):
            for to in others(h):
                y_copy(q, n, h, to, mine[h]).start()
            for e in range(slots):
                landing[q][n % ring[q], h, mine[h], e] = leaving[q][n % outs[q], h, mine[h], e]

    def tables():
        for h in range(2):
            for s in others(h):
                meta(h, s, s).wait_recv()
            for g in range(CHUNKS // GROUP):
                lane = lax.broadcasted_iota(jnp.int32, (share, width), 1)
                local = lax.broadcasted_iota(jnp.int32, (share, width), 0)
                goal = jnp.concatenate([
                    jnp.sum(jnp.where(lane == local + g * share, trecv[h * 4 + s][0:1], 0),
                            axis=1, keepdims=True) for s in range(sizes[h])], axis=0)
                index = lax.broadcasted_iota(jnp.int32, (span, 1), 0)
                valid = goal >= 0
                goal = jnp.where(valid, goal, 200)
                column = goal * 256 + index
                wide = (span, 2 * width)
                across = lax.broadcasted_iota(jnp.int32, wide, 1)
                down = lax.broadcasted_iota(jnp.int32, wide, 0)
                column_w = jnp.broadcast_to(column, wide)
                goal_w = jnp.broadcast_to(goal, wide)
                row = jnp.sum(jnp.where(across == down, column_w, 0), axis=0, keepdims=True)
                row_goal = jnp.sum(jnp.where(across == down, goal_w, 0), axis=0, keepdims=True)
                before = (row < column_w) & (across < span)
                rank = jnp.sum(jnp.where(before, 1, 0), axis=1, keepdims=True)
                joined = jnp.max(jnp.where(before & (row_goal == goal_w), 1, 0),
                                 axis=1, keepdims=True)
                entry = index + 1024 * joined
                entry = jnp.sum(jnp.where(rank == across, entry, 0), axis=0, keepdims=True)
                at = h * (CHUNKS // GROUP) + g
                order_v[at:at + 1] = entry
                found = jnp.where((goal == across[:, :width]) & valid, rank, -1)
                found = jnp.max(found, axis=0, keepdims=True)
                found = jnp.where(found < 0, span, found)
                spot_v[at:at + 1] = found
        for i, (source, into) in enumerate(((order_v, order), (spot_v, spot))):
            copy = pltpu.make_async_copy(source, into, tbl_sem.at[i])
            copy.start()
            copy.wait()

    def collect(q, n):
        for h in range(2):
            for s in others(h):
                y_copy(q, n, h, s, s).wait_recv()
            for s in range(sizes[h]):
                for e in range(slots):
                    work[q, h, s * share + e * GROUP + n % GROUP] = landing[q][n % ring[q], h, s, e]

    def densify(q, stream, g):
        for h in range(2):
            at = h * (CHUNKS // GROUP) + g

            def one(r, last):
                entry = order[at, r]
                value = work[q, h, entry & 1023]
                value = value + jnp.where(entry >= 1024, last, 0.0)
                scan[r] = value
                return value

            lax.fori_loop(0, span, one, jnp.zeros((half, low, width), jnp.float32), unroll=16)

            @pl.loop(0, sizes[1 - h])
            def _(o):
                @pl.loop(0, CHI_DEV, unroll=16)
                def _(e):
                    value = scan[spot[at, o * CHI_DEV + e]]
                    if g:
                        value = value + dense[stream, h, o, e]
                    dense[stream, h, o, e] = value

            if g and stream == 1:
                for to in others(1 - h):
                    z_copy(1, h, to, mine[1 - h]).start()

    def send_relay(q):
        for h in range(2):
            for right in (True, False):
                relay_copy(q, h, right, False).start()

    def send_merged(q):
        for h in range(2):
            i, after, across, before = around(h)
            mid = CHI_DEV // 2
            for right in (True, False):
                relay_copy(q, h, right, True).wait_recv()

            @pl.loop(0, mid, unroll=4)
            def _(e):
                dense[q, h, after, e] += zrecv[q, h, i, e]
                dense[q, h, before, mid + e] += zrecv[q, h, i, mid + e]
            z_copy(q, h, after, i).start()
            z_copy(q, h, before, i).start()

    def givers(q, h):
        i, after, across, before = around(h)
        return others(1 - h) if q == 1 else [after, before]

    def finish(q, store):
        for h in range(2):
            for s in givers(q, h):
                z_copy(q, h, s, s).wait_recv()
            own = mine[1 - h]

            @pl.loop(0, CHI_DEV, unroll=4)
            def _(e):
                total = dense[q, h, own, e]
                for s in givers(q, h):
                    total += zrecv[q, h, s, e]
                for k in range(half):
                    store(h * half + k, e, total[k])

    def store_early(k, e, value):
        out[k, e, 0:low] = value

    def store_late(k, e, value):
        out[k, e, low:rows] = value

    def store_final(k, e, value):
        final[k, e] = value

    def when(condition):
        return pl.when(condition)

    @pl.loop(0, 2 * rounds + 2 + LATER)
    def _(t):
        @when(t < rounds)
        def _():
            @when(t >= PBUFS)
            def _():
                for to in times():
                    early_copy(t - PBUFS, to, tau).wait_send()
            compute(t)

        @when(t == rounds - 1)
        def _():
            @pl.loop(0, rounds)
            def _(c):
                late_each(c, lambda copy: copy.start())

        @when(t < rounds)
        def _():
            send_y(1, t, t, timed)

            @pl.loop(0, per, unroll=4)
            def _(i):
                x_early[t % XRING, tau, i] = early[t % PBUFS, tau, i]

        @when((t >= 2) & (t < rounds + 2))
        def _():
            c = t - 2
            for s in times():
                early_copy(c, s, s).wait_recv()
            transform(x_early, c % XRING)
            send_y(0, c, c, freq)

        @when((t >= rounds + 2) & (t < 2 * rounds + 2) & (core == 1))
        def _():
            c = t - rounds - 2

            @pl.loop(0, per, unroll=4)
            def _(i):
                x_late[c, tau, i] = late[c, x, i]
            for s in times():
                late_copy(c, x, s).wait_recv()
            transform(x_late, c)
            send_y(1, c + rounds, c, freq)

        @when(t == 3)
        def _():
            tables()

        @when((t >= 2) & (t < rounds + 2))
        def _():
            collect(1, t - 2)

        @when(t == GROUP + 1)
        def _():
            densify(1, 2, 0)

        @when(t == rounds + 1)
        def _():
            densify(1, 2, 1)

        @when((t >= 4) & (t < rounds + 2))
        def _():
            collect(0, t - 4)

        @when(t == GROUP + 3)
        def _():
            densify(0, 0, 0)

        @when(t == rounds + 1)
        def _():
            send_relay(2)

        @when(t == rounds + 3)
        def _():
            collect(0, rounds - 2)
            collect(0, rounds - 1)
            densify(0, 0, 1)
            send_relay(0)
            send_merged(2)

        @when(t == jnp.where(core == 1, rounds + ZLATE, rounds + ZSOON))
        def _():
            send_merged(0)

        @when(t == rounds + FSTEP)
        def _():
            finish(2, store_final)
            back_each(lambda copy: copy.start())

        @when((t >= rounds + 2 + LATER) & (core == 1))
        def _():
            collect(1, t - 2 - LATER)

        @when((t == rounds + 1 + LATER + GROUP) & (core == 1))
        def _():
            densify(1, 1, 0)

    @when(core == 1)
    def _():
        densify(1, 1, 1)

    finish(0, store_early)

    @when(core == 1)
    def _():
        finish(1, store_late)

    @when(core == 0)
    def _():
        @pl.loop(0, CHI_DEV, unroll=4)
        def _(e):
            back[tau, e] = final[x, e]
        for s in times():
            back_copy(x, s).wait_recv()

        @pl.loop(0, CHI_DEV, unroll=2)
        def _(e):
            values = [back[s, e] for s in range(groups)]
            for k in range(freqs):
                total = weights[k, 0] * values[0]
                for s in range(1, groups):
                    total += weights[k, s] * values[s]
                out[k, e, low:rows] = total

    def drain_z(q):
        for h in range(2):
            for to in givers(q, h):
                z_copy(q, h, to, mine[1 - h]).wait_send()
            if q != 1:
                for right in (True, False):
                    relay_copy(q, h, right, False).wait_send()

    def drain_y(q):
        for h in range(2):
            for n in range(outs[q]):
                for to in others(h):
                    y_copy(q, n, h, to, mine[h]).wait_send()

    for h in range(2):
        for to in others(h):
            meta(h, to, mine[h]).wait_send()
    drain_z(2)
    drain_z(0)
    drain_y(0)
    drain_y(1)
    pl.when(core == 1)(lambda: drain_z(1))
    back_each(lambda copy: copy.wait_send())

    @pl.loop(0, rounds)
    def _(c):
        late_each(c, lambda copy: copy.wait_send())

    @pl.loop(rounds - PBUFS, rounds)
    def _(c):
        for to in times():
            early_copy(c, to, tau).wait_send()


def plan(target, owners, ny, nz):
    count = target.shape[0]
    per = count // CHUNKS
    each = CAP // CHUNKS
    index = jnp.arange(count, dtype=jnp.int32)
    key = target * 256 + index
    rank = jnp.sum((key[None, :] < key[:, None]).astype(jnp.int32), axis=1)
    at = jnp.arange(per)[None, :] * CHUNKS + jnp.arange(CHUNKS)[:, None]
    ordered = jnp.sum(jnp.where(rank == at[..., None], key, 0), axis=2)
    part = ordered & 255
    tile = ordered >> 8
    same = (tile[:, 1:] == tile[:, :-1]).astype(jnp.int32)
    none = jnp.zeros((CHUNKS, 1), jnp.int32)
    keep = jnp.concatenate([none, same], axis=1)
    last = 1 - jnp.concatenate([same, none], axis=1)
    owner = tile // CHI_DEV
    value = jnp.where(last != 0, tile - owner * CHI_DEV, -1)
    j = jnp.arange(owners * each, dtype=jnp.int32)
    d, m = j // each, j % each
    place = jnp.sum((owner[:, None, :] < d[None, :, None]).astype(jnp.int32), axis=2) + m
    within = jnp.arange(per, dtype=jnp.int32)
    hit = (place[..., None] == within) & (owner[:, None, :] == d[None, :, None])
    goal = jnp.sum(jnp.where(hit, value[:, None, :] + 1, 0), axis=2) - 1
    place = jnp.minimum(place, per - 1)
    goal = goal.reshape(CHUNKS // GROUP, GROUP, nz, ny, each)
    zs = jnp.arange(nz, dtype=jnp.int32)[:, None, None] * CHI_DEV
    ys = jnp.arange(ny, dtype=jnp.int32)[None, :, None] * CHI_DEV
    to_y = jnp.where(goal >= 0, goal + zs, -1).transpose(3, 0, 2, 4, 1).reshape(ny, -1)
    to_z = jnp.where(goal >= 0, goal + ys, -1).transpose(2, 0, 3, 4, 1).reshape(nz, -1)
    both = jnp.concatenate([to_y, to_z])
    both = jnp.pad(both, ((0, 0), (0, 128 - both.shape[1])))
    both = jnp.broadcast_to(both[:, None], (both.shape[0], 8, 128))
    steps = jnp.concatenate([part, keep, place], axis=1)
    steps = jnp.pad(steps, ((0, 0), (0, 128 - steps.shape[1])))
    return jnp.concatenate([both, steps[None]])


def body(occupied, virtual, cos_weights, pair_occ, pair_virt, partial_target_tile):
    owners = lax.axis_size("tile")
    groups = lax.axis_size("tau")
    size = occupied.shape[2]
    terms = pair_occ.shape[1]
    count = partial_target_tile.shape[0]
    freqs = cos_weights.shape[0]
    ny = 1
    while 2 * ny * 2 * ny <= owners:
        ny *= 2
    nz = owners // ny
    rows = size // groups
    per = count // CHUNKS
    slots = ny * (CAP // CHUNKS)
    half = freqs // 2
    low = rows // 2
    nx = groups // 2
    span = ny * slots * GROUP
    both = plan(partial_target_tile, owners, ny, nz)
    vmem = pl.BlockSpec(memory_space=pltpu.VMEM)
    dma = pltpu.SemaphoreType.DMA
    f32 = jnp.float32
    return pl.pallas_call(
        functools.partial(main_kernel, ny, nz, groups, terms),
        out_shape=jax.ShapeDtypeStruct((freqs, CHI_DEV, rows, size), f32),
        in_specs=[pl.BlockSpec(memory_space=pl.ANY)] * 6,
        out_specs=vmem,
        scratch_shapes=[
            pltpu.VMEM(occupied.shape[1:], occupied.dtype),
            pltpu.VMEM(virtual.shape[1:], virtual.dtype),
            pltpu.SMEM(cos_weights.shape, f32),
            pltpu.SMEM((terms, count), jnp.int32),
            pltpu.SMEM((terms, count), jnp.int32),
            pltpu.SMEM(both.shape[1:], jnp.int32),
            pltpu.VMEM((8,) + both.shape[1:], jnp.int32),
            pltpu.VMEM((PBUFS, groups, per, low, size), f32),
            pltpu.VMEM((CHUNKS, nx, per, low, size), f32),
            pltpu.VMEM((per, nx, low, size), f32),
            pltpu.VMEM((XRING, groups, per, low, size), f32),
            pltpu.VMEM((CHUNKS, groups, per, low, size), f32),
            pltpu.VMEM((per, freqs, low, size), f32),
            pltpu.VMEM((YBUFS[0], 2, ny, slots, half, low, size), f32),
            pltpu.VMEM((YBUFS[1], 2, ny, slots, half, low, size), f32),
            pltpu.VMEM((RINGS[0], 2, ny, slots, half, low, size), f32),
            pltpu.VMEM((RINGS[1], 2, ny, slots, half, low, size), f32),
            pltpu.VMEM((2, 2, span, half, low, size), f32),
            pltpu.VMEM((span + 1, half, low, size), f32),
            pltpu.VMEM((3, 2, ny, CHI_DEV, half, low, size), f32),
            pltpu.VMEM((3, 2, ny, CHI_DEV, half, low, size), f32),
            pltpu.VMEM((nx, CHI_DEV, low, size), f32),
            pltpu.VMEM((groups, CHI_DEV, low, size), f32),
            pltpu.VMEM((8, 8, size), jnp.int32),
            pltpu.VMEM((8, 2 * size), jnp.int32),
            pltpu.VMEM((8, size), jnp.int32),
            pltpu.SMEM((8, 2 * size), jnp.int32),
            pltpu.SMEM((8, size), jnp.int32),
            dma((PBUFS * groups,)),
            dma((XRING * groups,)),
            dma((CHUNKS * nx,)),
            dma((CHUNKS * groups,)),
            dma((sum(YBUFS) * 8,)),
            dma((sum(RINGS) * 8,)),
            dma((3 * 8,)),
            dma((3 * 8,)),
            dma((nx,)),
            dma((groups,)),
            dma((8,)),
            dma((8,)),
            dma((2,)),
            dma((2 * LOADS + 5,)),
        ],
        compiler_params=pltpu.CompilerParams(
            collective_id=0, has_side_effects=True, vmem_limit_bytes=67043328),
    )(cos_weights, pair_occ.T, pair_virt.T, both,
      occupied[0], virtual[0])


def solution(mesh):
    in_specs = (
        P("tau", "tile", None, None),
        P("tau", "tile", None, None),
        P(),
        P("tile", None),
        P("tile", None),
        P("tile"),
    )
    out_specs = P(None, "tile", "tau", None)
    return jax.shard_map(body, mesh=mesh, in_specs=in_specs, out_specs=out_specs, check_vma=False)
```
